32 devices in a mesh: dp: 8 (over y, x, core), tensor: 4 (over z).
Axes of the slice: x: 2, y: 2, z: 4, core: 2. Of those that a mesh axis runs over, the one named last changes fastest.
Arguments:
- tokens: bfloat16 [12288, 2048], P(('dp', 'tensor')), may hold values from -6 to 6
- segments: int32 [12288], P('dp'), may hold values from 0 to 4, as said below
- cotangent: bfloat16 [12288, 2048], P(('dp', 'tensor')), may hold values from -6 to 6
- ln1_gain: bfloat16 [2048], replicated, may hold values from 0.5 to 1.5
- ln1_shift: bfloat16 [2048], replicated, may hold values from -1.5 to 1.5
- w_query: bfloat16 [2048, 2048], P('dp', 'tensor'), may hold values from -0.1875 to 0.1875
- b_query: bfloat16 [2048], P('tensor'), may hold values from -1.5 to 1.5
- w_key: bfloat16 [2048, 2048], P('dp', 'tensor'), may hold values from -0.1875 to 0.1875
- w_value: bfloat16 [2048, 2048], P('dp', 'tensor'), may hold values from -0.125 to 0.125
- b_value: bfloat16 [2048], P('tensor'), may hold values from -1.5 to 1.5
- w_out: bfloat16 [2048, 2048], P('tensor', 'dp'), may hold values from -0.5 to 0.5
- b_out: bfloat16 [2048], replicated, may hold values from -1.5 to 1.5
- ln2_gain: bfloat16 [2048], replicated, may hold values from 0.5 to 1.5
- ln2_shift: bfloat16 [2048], replicated, may hold values from -1.5 to 1.5
- w_up: bfloat16 [2048, 8192], P('dp', 'tensor'), may hold values from -0.125 to 0.125
- b_up: bfloat16 [8192], P('tensor'), may hold values from -1.5 to 1.5
- w_down: bfloat16 [8192, 2048], P('tensor', 'dp'), may hold values from -0.0625 to 0.0625
- b_down: bfloat16 [2048], replicated, may hold values from -1.5 to 1.5
Outputs:
- output: bfloat16 [12288, 2048], P(('dp', 'tensor'))
- input_grad: bfloat16 [12288, 2048], P(('dp', 'tensor'))
- grad_ln1_gain: float32 [2048], replicated
- grad_ln1_shift: float32 [2048], replicated
- grad_w_query: float32 [2048, 2048], P('dp', 'tensor')
- grad_b_query: float32 [2048], P('tensor')
- grad_w_key: float32 [2048, 2048], P('dp', 'tensor')
- grad_w_value: float32 [2048, 2048], P('dp', 'tensor')
- grad_b_value: float32 [2048], P('tensor')
- grad_w_out: float32 [2048, 2048], P('tensor', 'dp')
- grad_b_out: float32 [2048], replicated
- grad_ln2_gain: float32 [2048], replicated
- grad_ln2_shift: float32 [2048], replicated
- grad_w_up: float32 [2048, 8192], P('dp', 'tensor')
- grad_b_up: float32 [8192], P('tensor')
- grad_w_down: float32 [8192, 2048], P('tensor', 'dp')
- grad_b_down: float32 [2048], replicated
The draws below stay inside these ranges and needn't reach their ends.
Inputs may be any that keep to these rules, and one draw needn't show every extreme that they name: Within each group of 1536 tokens the first 1024 have segment 0; the rest form 4 contiguous runs with segments 1 to 4 in rising order, each run 128 // 2 to 192 tokens long; in every group one run is exactly 192 long.
All inputs are finite; a program needn't handle non-finite values.
Results may differ from the reference program's by a relative error of at most 0.017.
Values may be sent and summed in bfloat16 or wider, within the bound.
A program may use at most 320 MiB of HBM per device.

```python
import math
import jax
import jax.numpy as jnp
from jax import lax

D = 2048
HEADS = 16
HDIM = 128
FF = 8192
PROMPT = 1024
CONT = 128
NCONT = 4
QBLK = 768
GROUP_TOK = 1536
TOKENS = 12288


def draw_segments(key, part):
    groups = TOKENS // GROUP_TOK
    pairs = NCONT // 2
    half_len = CONT // 2
    key_offset, key_pick, key_order = jax.random.split(jax.random.fold_in(key, 11), 3)
    offsets = jax.random.randint(key_offset, (groups, pairs), 0, half_len + 1)
    picked = jax.random.randint(key_pick, (groups, 1), 0, pairs)
    offsets = jnp.where(jnp.arange(pairs)[None, :] == picked, half_len, offsets)
    lengths = jnp.concatenate([CONT + offsets, CONT - offsets], axis=1).astype(jnp.int32)
    orders = jax.vmap(lambda order_key: jax.random.permutation(order_key, NCONT))(jax.random.split(key_order, groups))
    lengths = jnp.take_along_axis(lengths, orders, axis=1)
    run_ends = jnp.cumsum(lengths, axis=1)
    places = jnp.arange(NCONT * CONT, dtype=jnp.int32)
    cont_ids = 1 + jnp.sum((places[None, :, None] >= run_ends[:, None, :]).astype(jnp.int32), axis=2)
    prompt_ids = jnp.zeros((groups, PROMPT), jnp.int32)
    return jnp.concatenate([prompt_ids, cont_ids.astype(jnp.int32)], axis=1).reshape(TOKENS)


def level_of(stream_key, extent, cuts, least, high):
    def one(position, parts):
        steps = jax.random.uniform(jax.random.fold_in(jax.random.fold_in(stream_key, 6), position), (parts,), jnp.float32, least / len(cuts), high / len(cuts))
        return jnp.repeat(jnp.exp(steps), extent[position] // parts).reshape((-1,) + (1,) * (len(extent) - position - 1))

    loudness = one(*cuts[0])
    for cut in cuts[1:]:
        loudness = loudness * one(*cut)
    return loudness


def bell_draw(rng, extent, deviation, limit, cuts=(), kind=jnp.bfloat16):
    drawn = deviation * jax.random.normal(rng, extent, jnp.float32)
    if cuts:
        drawn = drawn * level_of(rng, extent, cuts, -0.22, 0.18)
    return jnp.clip(drawn, -limit, limit).astype(kind)


def setup_inputs(seed: int = 0) -> dict:
    streams_of = jax.random.split(jax.random.key(seed), 19)
    tokens = bell_draw(streams_of[0], (TOKENS, D), 1.0, 6.0, ((0, 32),))
    segments = draw_segments(jax.random.fold_in(streams_of[18], 71), 0)
    cotangent = bell_draw(streams_of[2], (TOKENS, D), 1.0, 6.0, ((0, 32),))
    ln1_gain = jnp.clip(1.0 + 0.1 * jax.random.normal(streams_of[3], (D,), jnp.float32), 0.5, 1.5).astype(jnp.bfloat16)
    ln1_shift = bell_draw(streams_of[4], (D,), 0.3, 1.5)
    w_query = bell_draw(streams_of[5], (D, D), (D // 2) ** -0.5, 0.1875, ((0, 8), (1, 4)))
    b_query = bell_draw(streams_of[6], (D,), 0.3, 1.5, ((0, 4),))
    w_key = bell_draw(streams_of[7], (D, D), (D // 2) ** -0.5, 0.1875, ((0, 8), (1, 4)))
    w_value = bell_draw(streams_of[8], (D, D), D ** -0.5, 0.125, ((0, 8), (1, 4)))
    b_value = bell_draw(streams_of[9], (D,), 0.3, 1.5, ((0, 4),))
    w_out = bell_draw(streams_of[10], (D, D), (D // 16) ** -0.5, 0.5, ((0, 4), (1, 8)))
    b_out = bell_draw(streams_of[11], (D,), 0.3, 1.5)
    ln2_gain = jnp.clip(1.0 + 0.1 * jax.random.normal(streams_of[12], (D,), jnp.float32), 0.5, 1.5).astype(jnp.bfloat16)
    ln2_shift = bell_draw(streams_of[13], (D,), 0.3, 1.5)
    w_up = bell_draw(streams_of[14], (D, FF), D ** -0.5, 0.125, ((0, 8), (1, 4)))
    b_up = bell_draw(streams_of[15], (FF,), 0.3, 1.5, ((0, 4),))
    w_down = bell_draw(streams_of[16], (FF, D), FF ** -0.5, 0.0625, ((0, 4), (1, 8)))
    b_down = bell_draw(streams_of[17], (D,), 0.3, 1.5)
    return {"tokens": tokens, "segments": segments, "cotangent": cotangent, "ln1_gain": ln1_gain, "ln1_shift": ln1_shift, "w_query": w_query, "b_query": b_query, "w_key": w_key, "w_value": w_value, "b_value": b_value, "w_out": w_out, "b_out": b_out, "ln2_gain": ln2_gain, "ln2_shift": ln2_shift, "w_up": w_up, "b_up": b_up, "w_down": w_down, "b_down": b_down}


@jax.custom_vjp
def low(v):
    return lax.optimization_barrier(v.astype(jnp.bfloat16)).astype(jnp.float32)

@jax.custom_vjp
def low_back(v):
    return v

def low_keep(v):
    return (low(v), None)

def low_pass(kept, grad):
    return (grad,)

def back_keep(v):
    return (v, None)

def back_low(kept, grad):
    return (low(grad),)
low.defvjp(low_keep, low_pass)
low_back.defvjp(back_keep, back_low)
HIGH = lax.Precision.HIGHEST
EPS = 1e-05
NEG = -1e+30

def layer_norm(values, norm_gain, norm_shift):
    row_mean = lax.optimization_barrier(jnp.mean(values, axis=-1, keepdims=True))
    centred = values - row_mean
    row_var = lax.optimization_barrier(jnp.mean(centred * centred, axis=-1, keepdims=True))
    return centred * lax.rsqrt(row_var + EPS) * norm_gain + norm_shift

def matmul(left_side, right_side):
    return jnp.dot(left_side, right_side, precision=HIGH, preferred_element_type=jnp.float32)

def visible(segments, first_row, row_count, key_end):
    query_pos = first_row + jnp.arange(row_count)
    key_pos = jnp.arange(key_end)
    seg_query = segments[first_row:first_row + row_count]
    seg_key = segments[:key_end]
    causal = key_pos[None, :] <= query_pos[:, None]
    shared = (seg_key[None, :] == seg_query[:, None]) | (seg_key[None, :] == 0)
    return causal & shared

def attend(queries, key_rows, value_rows, allowed):
    scores = jnp.einsum('qhd,khd->hqk', queries, key_rows, precision=HIGH)
    scores = low_back(scores)
    scores = jnp.where(allowed[None], scores, NEG)
    weights = jax.nn.softmax(scores, axis=-1)
    return jnp.einsum('hqk,khd->qhd', low(weights), value_rows, precision=HIGH)

def forward_group(param_set, group_in, segments):
    gain_one, shift_one, w_q, b_q, w_k, w_v, b_v, w_o, b_o, gain_two, shift_two, w_u, b_u, w_d, b_d = param_set
    group_len = group_in.shape[0]
    h_one = low(layer_norm(group_in, gain_one, shift_one))
    queries = low(low_back((matmul(h_one, w_q) + b_q) / math.sqrt(HDIM)))
    key_rows = low(low_back(matmul(h_one, w_k)))
    value_rows = low(low_back(matmul(h_one, w_v) + b_v))
    query3 = queries.reshape(group_len, HEADS, HDIM)
    key3 = key_rows.reshape(group_len, HEADS, HDIM)
    value3 = value_rows.reshape(group_len, HEADS, HDIM)
    pieces = []
    for block in range(group_len // QBLK):
        first_row = block * QBLK
        key_end = first_row + QBLK
        allowed = visible(segments, first_row, QBLK, key_end)
        pieces.append(jax.checkpoint(attend)(query3[first_row:key_end], key3[:key_end], value3[:key_end], allowed))
    attended = low_back(low(jnp.concatenate(pieces, axis=0).reshape(group_len, HEADS * HDIM)))
    mixed = low_back(matmul(attended, w_o) + b_o)
    resid = group_in + mixed
    h_two = low(layer_norm(resid, gain_two, shift_two))
    pre_act = low_back(matmul(h_two, w_u) + b_u)
    activated = low(jax.nn.gelu(pre_act, approximate=False))
    return resid + matmul(activated, w_d) + b_d

def reference(tokens, segments, cotangent, ln1_gain, ln1_shift, w_query, b_query, w_key, w_value, b_value, w_out, b_out, ln2_gain, ln2_shift, w_up, b_up, w_down, b_down):
    param_set = tuple((item.astype(jnp.float32) for item in (ln1_gain, ln1_shift, w_query, b_query, w_key, w_value, b_value, w_out, b_out, ln2_gain, ln2_shift, w_up, b_up, w_down, b_down)))
    groups = tokens.shape[0] // GROUP_TOK
    token_groups = tokens.astype(jnp.float32).reshape(groups, GROUP_TOK, D)
    seg_groups = segments.reshape(groups, GROUP_TOK)
    cot_groups = cotangent.astype(jnp.float32).reshape(groups, GROUP_TOK, D)

    def one_group(grad_sums, inputs_here):
        group_x, group_seg, group_cot = inputs_here
        result, pullback = jax.vjp(lambda params_in, group_in: forward_group(params_in, group_in, group_seg), param_set, group_x)
        grad_params, grad_x = pullback(group_cot)
        grad_sums = jax.tree.map(jnp.add, grad_sums, grad_params)
        return (grad_sums, (result.astype(jnp.bfloat16), grad_x.astype(jnp.bfloat16)))
    zero_sums = jax.tree.map(jnp.zeros_like, param_set)
    sums, (out_rows, grad_rows) = lax.scan(one_group, zero_sums, (token_groups, seg_groups, cot_groups))
    return (out_rows.reshape(-1, D), grad_rows.reshape(-1, D), sums[0], sums[1], sums[2], sums[3], sums[4], sums[5], sums[6], sums[7], sums[8], sums[9], sums[10], sums[11], sums[12], sums[13], sums[14])
```

```python
import math

import jax
import jax.numpy as jnp
from jax import lax
from jax.sharding import PartitionSpec as P

HDIM = 128
QBLK = 768


EPS = 1e-05
NEG = -1e30


def layer_norm(values, norm_gain, norm_shift):
    row_mean = jnp.mean(values, axis=-1, keepdims=True)
    centred = values - row_mean
    row_var = jnp.mean(centred * centred, axis=-1, keepdims=True)
    return centred * lax.rsqrt(row_var + EPS) * norm_gain + norm_shift


def gelu_exact(values):
    return jax.nn.gelu(values, approximate=False)


def row_dot(left_side, right_side):
    return jnp.dot(left_side, right_side, preferred_element_type=jnp.float32)


def left_dot(left_side, right_side):
    return lax.dot_general(
        left_side, right_side, (((0,), (0,)), ((), ())), preferred_element_type=jnp.float32
    )


def back_dot(left_side, right_side):
    return lax.dot_general(
        left_side, right_side, (((1,), (1,)), ((), ())), preferred_element_type=jnp.float32
    )


def visible(segments, first_row, row_count, key_end):
    query_pos = first_row + jnp.arange(row_count)
    key_pos = jnp.arange(key_end)
    seg_query = segments[first_row : first_row + row_count]
    seg_key = segments[:key_end]
    causal = key_pos[None, :] <= query_pos[:, None]
    shared = (seg_key[None, :] == seg_query[:, None]) | (seg_key[None, :] == 0)
    return causal & shared


def attend_block(queries, key_rows, value_rows, allowed):
    scores = jnp.einsum("qhd,khd->hqk", queries, key_rows, preferred_element_type=jnp.float32)
    scores = jnp.where(allowed[None], scores, NEG)
    row_top = jnp.max(scores, axis=-1, keepdims=True)
    raised = jnp.exp(scores - row_top)
    row_total = jnp.sum(raised, axis=-1, keepdims=True)
    weights = raised / row_total
    mixed = jnp.einsum(
        "hqk,khd->qhd", weights.astype(jnp.bfloat16), value_rows, preferred_element_type=jnp.float32
    )
    return (mixed.astype(jnp.bfloat16), row_top + jnp.log(row_total))


def attend_back(queries, key_rows, value_rows, grad_out, log_total, allowed):
    scores = jnp.einsum("qhd,khd->hqk", queries, key_rows, preferred_element_type=jnp.float32)
    weights = jnp.where(allowed[None], jnp.exp(scores - log_total), 0.0)
    grad_weights = jnp.einsum(
        "qhd,khd->hqk", grad_out, value_rows, preferred_element_type=jnp.float32
    )
    inner = jnp.sum(weights * grad_weights, axis=-1, keepdims=True)
    grad_scores = (weights * (grad_weights - inner)).astype(jnp.bfloat16)
    grad_query = jnp.einsum(
        "hqk,khd->qhd", grad_scores, key_rows, preferred_element_type=jnp.float32
    )
    grad_key = jnp.einsum("hqk,qhd->khd", grad_scores, queries, preferred_element_type=jnp.float32)
    grad_value = jnp.einsum(
        "hqk,qhd->khd", weights.astype(jnp.bfloat16), grad_out, preferred_element_type=jnp.float32
    )
    return (grad_query, grad_key, grad_value)


def on_device(
    tokens,
    segments,
    cotangent,
    ln1_gain,
    ln1_shift,
    w_query,
    b_query,
    w_key,
    w_value,
    b_value,
    w_out,
    b_out,
    ln2_gain,
    ln2_shift,
    w_up,
    b_up,
    w_down,
    b_down,
):
    score_scale = 1.0 / math.sqrt(HDIM)
    full_query, full_key, full_value, full_out, full_up, full_down = (
        lax.all_gather(w_query, "dp", axis=0, tiled=True),
        lax.all_gather(w_key, "dp", axis=0, tiled=True),
        lax.all_gather(w_value, "dp", axis=0, tiled=True),
        lax.all_gather(w_out, "dp", axis=1, tiled=True),
        lax.all_gather(w_up, "dp", axis=0, tiled=True),
        lax.all_gather(w_down, "dp", axis=1, tiled=True),
    )
    group_len = segments.shape[0]
    head_cols = full_query.shape[1]
    heads_here = head_cols // HDIM
    block_count = group_len // QBLK
    inputs = tokens.astype(jnp.float32)
    normed_one, norm_one_back = jax.vjp(
        layer_norm, inputs, ln1_gain.astype(jnp.float32), ln1_shift.astype(jnp.float32)
    )
    h_one = normed_one.astype(jnp.bfloat16)
    h_one_full = lax.all_gather(h_one, "tensor", axis=0, tiled=True)
    w_qkv = jnp.concatenate([full_query, full_key, full_value], axis=1)
    w_kv = w_qkv[:, head_cols:]
    projected = row_dot(h_one_full, w_qkv)
    queries = ((projected[:, :head_cols] + b_query.astype(jnp.float32)) * score_scale).astype(
        jnp.bfloat16
    )
    key_rows = projected[:, head_cols : 2 * head_cols].astype(jnp.bfloat16)
    value_rows = (projected[:, 2 * head_cols :] + b_value.astype(jnp.float32)).astype(jnp.bfloat16)
    query3 = queries.reshape(group_len, heads_here, HDIM)
    key3 = key_rows.reshape(group_len, heads_here, HDIM)
    value3 = value_rows.reshape(group_len, heads_here, HDIM)
    pieces = []
    totals = []
    for block in range(block_count):
        first_row = block * QBLK
        key_end = first_row + QBLK
        allowed = visible(segments, first_row, QBLK, key_end)
        mixed_block, log_total = attend_block(
            query3[first_row:key_end], key3[:key_end], value3[:key_end], allowed
        )
        pieces.append(mixed_block)
        totals.append(log_total)
    attended = jnp.concatenate(pieces, axis=0).reshape(group_len, head_cols)
    resid = (
        inputs
        + lax.psum_scatter(row_dot(attended, full_out), "tensor", scatter_dimension=0, tiled=True)
        + b_out.astype(jnp.float32)
    )
    normed_two, norm_two_back = jax.vjp(
        layer_norm, resid, ln2_gain.astype(jnp.float32), ln2_shift.astype(jnp.float32)
    )
    h_two = normed_two.astype(jnp.bfloat16)
    h_two_full = lax.all_gather(h_two, "tensor", axis=0, tiled=True)
    pre_act = row_dot(h_two_full, full_up) + b_up.astype(jnp.float32)
    activated, gelu_back = jax.vjp(gelu_exact, pre_act)
    act_low = activated.astype(jnp.bfloat16)
    output = (
        resid
        + lax.psum_scatter(
            row_dot(act_low, full_down).astype(jnp.bfloat16),
            "tensor",
            scatter_dimension=0,
            tiled=True,
        ).astype(jnp.float32)
        + b_down.astype(jnp.float32)
    ).astype(jnp.bfloat16)
    grad_y = cotangent.astype(jnp.float32)
    grad_y_full = lax.all_gather(cotangent, "tensor", axis=0, tiled=True)
    grad_down = left_dot(act_low, grad_y_full)
    grad_act = back_dot(grad_y_full, full_down)
    grad_pre = gelu_back(grad_act)[0].astype(jnp.bfloat16)
    grad_bias_up = jnp.sum(grad_pre.astype(jnp.float32), axis=0)
    grad_up = left_dot(h_two_full, grad_pre)
    grad_h_two = lax.psum_scatter(
        back_dot(grad_pre, full_up), "tensor", scatter_dimension=0, tiled=True
    )
    grad_resid_norm, grad_gain_two, grad_shift_two = norm_two_back(grad_h_two)
    grad_resid = grad_y + grad_resid_norm
    grad_mix = grad_resid.astype(jnp.bfloat16)
    grad_bias_out = jnp.sum(grad_mix.astype(jnp.float32), axis=0)
    grad_bias_down = jnp.sum(grad_y, axis=0)
    grad_mix_full = lax.all_gather(grad_mix, "tensor", axis=0, tiled=True)
    grad_out_w = left_dot(attended, grad_mix_full)
    grad_att = (
        back_dot(grad_mix_full, full_out).astype(jnp.bfloat16).reshape(group_len, heads_here, HDIM)
    )
    grad_key_sum = jnp.zeros((group_len, heads_here, HDIM), jnp.float32)
    grad_value_sum = jnp.zeros((group_len, heads_here, HDIM), jnp.float32)
    query_grads = []
    for block in range(block_count):
        first_row = block * QBLK
        key_end = first_row + QBLK
        allowed = visible(segments, first_row, QBLK, key_end)
        grad_q_block, grad_k_part, grad_v_part = attend_back(
            query3[first_row:key_end],
            key3[:key_end],
            value3[:key_end],
            grad_att[first_row:key_end],
            totals[block],
            allowed,
        )
        query_grads.append(grad_q_block.astype(jnp.bfloat16))
        grad_key_sum = grad_key_sum.at[:key_end].add(grad_k_part)
        grad_value_sum = grad_value_sum.at[:key_end].add(grad_v_part)
    grad_q = jnp.concatenate(query_grads, axis=0).reshape(group_len, head_cols)
    grad_k = grad_key_sum.reshape(group_len, head_cols).astype(jnp.bfloat16)
    grad_v = grad_value_sum.reshape(group_len, head_cols).astype(jnp.bfloat16)
    grad_qkv = jnp.concatenate([grad_q, grad_k, grad_v], axis=1)
    grad_qkv_w = left_dot(h_one_full, grad_qkv)
    grad_wq = grad_qkv_w[:, :head_cols] * score_scale
    grad_wk = grad_qkv_w[:, head_cols : 2 * head_cols]
    grad_wv = grad_qkv_w[:, 2 * head_cols :]
    grad_bias_query = jnp.sum(grad_q.astype(jnp.float32), axis=0) * score_scale
    grad_bias_value = jnp.sum(grad_v.astype(jnp.float32), axis=0)
    grad_h_one = lax.psum_scatter(
        (
            back_dot(grad_qkv[:, :head_cols], full_query) * score_scale
            + back_dot(grad_qkv[:, head_cols:], w_kv)
        ).astype(jnp.bfloat16),
        "tensor",
        scatter_dimension=0,
        tiled=True,
    ).astype(jnp.float32)
    grad_in_norm, grad_gain_one, grad_shift_one = norm_one_back(grad_h_one)
    input_grad = (grad_resid + grad_in_norm).astype(jnp.bfloat16)
    sent_query, sent_key, sent_value, sent_out, sent_up, sent_down = (
        lax.psum_scatter(
            grad_wq.astype(jnp.bfloat16), "dp", scatter_dimension=0, tiled=True
        ).astype(jnp.float32),
        lax.psum_scatter(
            grad_wk.astype(jnp.bfloat16), "dp", scatter_dimension=0, tiled=True
        ).astype(jnp.float32),
        lax.psum_scatter(
            grad_wv.astype(jnp.bfloat16), "dp", scatter_dimension=0, tiled=True
        ).astype(jnp.float32),
        lax.psum_scatter(
            grad_out_w.astype(jnp.bfloat16), "dp", scatter_dimension=1, tiled=True
        ).astype(jnp.float32),
        lax.psum_scatter(
            grad_up.astype(jnp.bfloat16), "dp", scatter_dimension=0, tiled=True
        ).astype(jnp.float32),
        lax.psum_scatter(
            grad_down.astype(jnp.bfloat16), "dp", scatter_dimension=1, tiled=True
        ).astype(jnp.float32),
    )
    summed_query, summed_value, summed_up = lax.psum(
        (grad_bias_query, grad_bias_value, grad_bias_up), "dp"
    )
    gain_one_sum, shift_one_sum, gain_two_sum, shift_two_sum, bias_out_sum, bias_down_sum = (
        lax.psum(
            (
                grad_gain_one,
                grad_shift_one,
                grad_gain_two,
                grad_shift_two,
                grad_bias_out,
                grad_bias_down,
            ),
            ("dp", "tensor"),
        )
    )
    return (
        output,
        input_grad,
        gain_one_sum,
        shift_one_sum,
        sent_query,
        summed_query,
        sent_key,
        sent_value,
        summed_value,
        sent_out,
        bias_out_sum,
        gain_two_sum,
        shift_two_sum,
        sent_up,
        summed_up,
        sent_down,
        bias_down_sum,
    )


def power_of_two(count):
    return count > 0 and count & (count - 1) == 0


def mirrored(value, count):
    bits = count.bit_length() - 1
    out = 0 * value
    for bit in range(bits):
        out = out + ((value >> bit) & 1) * (1 << (bits - 1 - bit))
    return out


class Links:
    def __init__(self, mesh):
        self.cols = mesh.shape["tensor"]
        self.ranks = self.cols
        self.halves = mesh.shape["dp"] // self.ranks
        dp_index = lax.axis_index("dp")
        self.half = dp_index // self.ranks
        self.rank = dp_index % self.ranks
        self.col = lax.axis_index("tensor")
        self.quarter = mirrored(self.rank, self.ranks)

    def moved(self, values, target):
        pairs = []
        for half in range(self.halves):
            for rank in range(self.ranks):
                for col in range(self.cols):
                    to_half, to_rank, to_col = target(half, rank, col)
                    pairs.append(
                        (
                            (half * self.ranks + rank) * self.cols + col,
                            (to_half * self.ranks + to_rank) * self.cols + to_col,
                        )
                    )
        return lax.ppermute(values, ("dp", "tensor"), pairs)

    def swap(self, values):
        return self.moved(
            values, lambda half, rank, col: (half, mirrored(col, self.cols), mirrored(rank, self.ranks))
        )

    def rank_pair(self, values, bit):
        return self.moved(values, lambda half, rank, col: (half, rank ^ bit, col))

    def half_pair(self, values, bit):
        return self.moved(values, lambda half, rank, col: (half ^ bit, rank, col))

    def rank_bits(self):
        return [1 << place for place in range(self.ranks.bit_length() - 1)]

    def gather_rows(self, piece):
        pieces = {0: piece}
        for bit in reversed(self.rank_bits()):
            for at in list(pieces):
                pieces[at | bit] = self.rank_pair(pieces[at], bit)
        return [pieces[at] for at in range(self.ranks)]

    def scatter_rows(self, pieces):
        sums = dict(enumerate(pieces))
        for bit in self.rank_bits():
            for at in [item for item in sums if item & bit]:
                arrived = self.rank_pair(sums.pop(at).astype(jnp.bfloat16), bit)
                sums[at ^ bit] = sums[at ^ bit] + arrived.astype(jnp.float32)
        return sums[0]

    def half_order(self, values, axis):
        if self.halves == 1:
            return values
        width = values.shape[axis] // self.halves
        return jnp.concatenate(
            [
                lax.dynamic_slice_in_dim(values, (self.half ^ at) * width, width, axis)
                for at in range(self.halves)
            ],
            axis=axis,
        )

    def row_order(self, pieces):
        stacked = jnp.concatenate(pieces, axis=0)
        rows = pieces[0].shape[0]
        return jnp.concatenate(
            [
                lax.dynamic_slice_in_dim(
                    stacked, mirrored(at ^ self.quarter, self.ranks) * rows, rows, 0
                )
                for at in range(self.ranks)
            ],
            axis=0,
        )

    def piece_order(self, values):
        rows = values.shape[0] // self.ranks
        return [
            lax.dynamic_slice_in_dim(
                values, (self.quarter ^ mirrored(at, self.ranks)) * rows, rows, 0
            )
            for at in range(self.ranks)
        ]

    def rank_groups(self):
        return [
            [half * self.ranks + rank for rank in range(self.ranks)] for half in range(self.halves)
        ]

    def spread(self, shard, hidden_axis):
        other = 1 - hidden_axis
        part = lax.all_to_all(
            shard, "dp", hidden_axis, other, axis_index_groups=self.rank_groups(), tiled=True
        )
        part = lax.all_gather(part, "tensor", axis=hidden_axis, tiled=True)
        parts = {0: part}
        bit = self.halves // 2
        while bit:
            for at in list(parts):
                parts[at | bit] = self.half_pair(parts[at], bit)
            bit //= 2
        return jnp.concatenate([parts[at] for at in range(self.halves)], axis=other)

    def collect(self, grad, hidden_axis):
        other = 1 - hidden_axis
        width = grad.shape[other] // self.halves
        sums = {
            at: lax.slice_in_dim(grad, at * width, (at + 1) * width, axis=other)
            for at in range(self.halves)
        }
        bit = 1
        while bit < self.halves:
            for at in [item for item in sums if item & bit]:
                arrived = self.half_pair(sums.pop(at).astype(jnp.bfloat16), bit)
                sums[at ^ bit] = sums[at ^ bit] + arrived.astype(jnp.float32)
            bit *= 2
        part = lax.psum_scatter(
            sums[0].astype(jnp.bfloat16), "tensor", scatter_dimension=hidden_axis, tiled=True
        )
        return lax.all_to_all(
            part, "dp", other, hidden_axis, axis_index_groups=self.rank_groups(), tiled=True
        ).astype(jnp.float32)

    def rank_part(self, values):
        width = values.shape[0] // self.ranks
        return lax.dynamic_slice_in_dim(values, self.rank * width, width, 0)

    def rank_slots(self, values):
        mine = (jnp.arange(self.ranks) == self.rank).astype(values.dtype)
        blocks = values.reshape(self.cols, 1, -1)
        return (blocks * mine[None, :, None]).reshape(-1)


def swapped_on_device(
    mesh,
    tokens,
    segments,
    cotangent,
    ln1_gain,
    ln1_shift,
    w_query,
    b_query,
    w_key,
    w_value,
    b_value,
    w_out,
    b_out,
    ln2_gain,
    ln2_shift,
    w_up,
    b_up,
    w_down,
    b_down,
):
    links = Links(mesh)
    ranks, cols = links.ranks, links.cols
    score_scale = 1.0 / math.sqrt(HDIM)
    group_len = segments.shape[0]
    head_cols = w_query.shape[1]
    heads_here = head_cols // HDIM
    sub_cols = head_cols // ranks
    block_count = group_len // QBLK
    f32 = jnp.float32
    low = jnp.bfloat16

    tokens = links.half_order(links.swap(tokens), 1)
    segments = links.swap(segments)

    w_qkv_shard = jnp.concatenate(
        [item.reshape(-1, ranks, sub_cols) for item in (w_query, w_key, w_value)], axis=2
    ).reshape(w_query.shape[0], -1)
    biases = jnp.concatenate([links.rank_part(item) for item in (b_query, b_value, b_up)])
    biases = lax.all_gather(biases.astype(f32), "tensor", axis=0, tiled=False)
    bias_query = biases[:, :sub_cols].reshape(-1)
    bias_value = biases[:, sub_cols : 2 * sub_cols].reshape(-1)
    bias_up = biases[:, 2 * sub_cols :].reshape(-1)
    full_qkv = links.spread(w_qkv_shard, 1)
    full_out = links.spread(w_out, 0)
    full_up = links.spread(w_up, 1)
    full_down = links.spread(w_down, 0)

    gain_one, shift_one, gain_two, shift_two, out_bias, down_bias = (
        links.half_order(item.astype(f32), 0)
        for item in (ln1_gain, ln1_shift, ln2_gain, ln2_shift, b_out, b_down)
    )

    inputs = tokens.astype(f32)
    normed_one, norm_one_back = jax.vjp(layer_norm, inputs, gain_one, shift_one)
    h_one_pieces = links.gather_rows(normed_one.astype(low))
    projected = links.row_order([row_dot(piece, full_qkv) for piece in h_one_pieces])
    projected = projected.reshape(group_len, heads_here, 3, HDIM)
    query3 = (
        (projected[:, :, 0] + bias_query.reshape(heads_here, HDIM)) * score_scale
    ).astype(low)
    key3 = projected[:, :, 1].astype(low)
    value3 = (projected[:, :, 2] + bias_value.reshape(heads_here, HDIM)).astype(low)
    pieces = []
    totals = []
    for block in range(block_count):
        first_row = block * QBLK
        key_end = first_row + QBLK
        allowed = visible(segments, first_row, QBLK, key_end)
        mixed_block, log_total = attend_block(
            query3[first_row:key_end], key3[:key_end], value3[:key_end], allowed
        )
        pieces.append(mixed_block)
        totals.append(log_total)
    attended = jnp.concatenate(pieces, axis=0).reshape(group_len, head_cols)
    attended_pieces = links.piece_order(attended)
    resid = (
        inputs
        + links.scatter_rows([row_dot(piece, full_out) for piece in attended_pieces])
        + out_bias
    )
    normed_two, norm_two_back = jax.vjp(layer_norm, resid, gain_two, shift_two)
    h_two = jnp.concatenate(links.gather_rows(normed_two.astype(low)), axis=0)
    pre_act = row_dot(h_two, full_up) + bias_up
    activated, gelu_back = jax.vjp(gelu_exact, pre_act)
    act_low = activated.astype(low)
    rows = tokens.shape[0]
    output = (
        resid
        + links.scatter_rows(
            [row_dot(act_low[at * rows : (at + 1) * rows], full_down) for at in range(ranks)]
        )
        + down_bias
    ).astype(low)
    output = links.swap(links.half_order(output, 1))

    grad_y_low = links.half_order(links.swap(cotangent), 1)
    grad_y = grad_y_low.astype(f32)
    grad_y_full = jnp.concatenate(links.gather_rows(grad_y_low), axis=0)
    sent_down = links.collect(left_dot(act_low, grad_y_full), 0)
    grad_act = back_dot(grad_y_full, full_down)
    grad_pre = gelu_back(grad_act)[0].astype(low)
    grad_bias_up = jnp.sum(grad_pre.astype(f32), axis=0)
    sent_up = links.collect(left_dot(h_two, grad_pre), 1)
    grad_h_two = links.scatter_rows(
        [back_dot(grad_pre[at * rows : (at + 1) * rows], full_up) for at in range(ranks)]
    )
    grad_resid_norm, grad_gain_two, grad_shift_two = norm_two_back(grad_h_two)
    grad_resid = grad_y + grad_resid_norm
    grad_mix = grad_resid.astype(low)
    grad_bias_out = jnp.sum(grad_mix.astype(f32), axis=0)
    grad_bias_down = jnp.sum(grad_y, axis=0)
    grad_mix_pieces = links.gather_rows(grad_mix)
    grad_mix_full = jnp.concatenate(grad_mix_pieces, axis=0)
    sent_out = links.collect(
        left_dot(jnp.concatenate(attended_pieces, axis=0), grad_mix_full), 0
    )
    grad_att = links.row_order(
        [back_dot(piece, full_out).astype(low) for piece in grad_mix_pieces]
    ).reshape(group_len, heads_here, HDIM)
    grad_key_sum = jnp.zeros((group_len, heads_here, HDIM), f32)
    grad_value_sum = jnp.zeros((group_len, heads_here, HDIM), f32)
    query_grads = []
    for block in range(block_count):
        first_row = block * QBLK
        key_end = first_row + QBLK
        allowed = visible(segments, first_row, QBLK, key_end)
        grad_q_block, grad_k_part, grad_v_part = attend_back(
            query3[first_row:key_end],
            key3[:key_end],
            value3[:key_end],
            grad_att[first_row:key_end],
            totals[block],
            allowed,
        )
        query_grads.append(grad_q_block.astype(low))
        grad_key_sum = grad_key_sum.at[:key_end].add(grad_k_part)
        grad_value_sum = grad_value_sum.at[:key_end].add(grad_v_part)
    grad_q = jnp.concatenate(query_grads, axis=0)
    grad_k = grad_key_sum.astype(low)
    grad_v = grad_value_sum.astype(low)
    grad_bias_query = jnp.sum(grad_q.astype(f32), axis=0).reshape(-1) * score_scale
    grad_bias_value = jnp.sum(grad_v.astype(f32), axis=0).reshape(-1)
    grad_qkv = jnp.stack([grad_q, grad_k, grad_v], axis=2).reshape(group_len, 3 * head_cols)
    grad_pieces = links.piece_order(grad_qkv)
    scales = jnp.tile(
        jnp.concatenate([jnp.full((HDIM,), score_scale, f32), jnp.ones((2 * HDIM,), f32)]),
        heads_here,
    )
    grad_w_qkv = left_dot(
        jnp.concatenate(h_one_pieces, axis=0), jnp.concatenate(grad_pieces, axis=0)
    )
    sent_qkv = links.collect(grad_w_qkv * scales, 1).reshape(w_query.shape[0], ranks, 3, sub_cols)
    sent_query, sent_key, sent_value = (
        sent_qkv[:, :, at].reshape(w_query.shape) for at in range(3)
    )
    grad_q_pieces = links.piece_order(grad_q.reshape(group_len, head_cols))
    grad_kv_pieces = links.piece_order(
        jnp.stack([grad_k, grad_v], axis=2).reshape(group_len, 2 * head_cols)
    )
    split = full_qkv.reshape(full_qkv.shape[0], heads_here, 3, HDIM)
    only_query = split[:, :, 0].reshape(full_qkv.shape[0], head_cols)
    only_kv = split[:, :, 1:].reshape(full_qkv.shape[0], 2 * head_cols)
    grad_h_one = links.scatter_rows(
        [
            back_dot(q_piece, only_query) * score_scale + back_dot(kv_piece, only_kv)
            for q_piece, kv_piece in zip(grad_q_pieces, grad_kv_pieces)
        ]
    )
    grad_in_norm, grad_gain_one, grad_shift_one = norm_one_back(grad_h_one)
    input_grad = (grad_resid + grad_in_norm).astype(low)
    input_grad = links.swap(links.half_order(input_grad, 1))

    def my_block(values):
        width = values.shape[0] // cols
        return lax.dynamic_slice_in_dim(values, links.col * width, width, 0)

    early = lax.psum(
        (
            links.rank_slots(grad_bias_up),
            links.half_order(grad_gain_two, 0),
            links.half_order(grad_shift_two, 0),
            links.half_order(grad_bias_out, 0),
            links.half_order(grad_bias_down, 0),
        ),
        ("dp", "tensor"),
    )
    late = lax.psum(
        (
            links.rank_slots(grad_bias_query),
            links.rank_slots(grad_bias_value),
            links.half_order(grad_gain_one, 0),
            links.half_order(grad_shift_one, 0),
        ),
        ("dp", "tensor"),
    )
    return (
        output,
        input_grad,
        late[2],
        late[3],
        sent_query,
        my_block(late[0]),
        sent_key,
        sent_value,
        my_block(late[1]),
        sent_out,
        early[3],
        early[1],
        early[2],
        sent_up,
        my_block(early[0]),
        sent_down,
        early[4],
    )


def can_swap(mesh, head_cols):
    ranks = mesh.shape["tensor"]
    dp_size = mesh.shape["dp"]
    if dp_size % ranks or not power_of_two(ranks) or not power_of_two(dp_size // ranks):
        return False
    return head_cols % (ranks * HDIM) == 0


def either_on_device(mesh):
    def run(*arrays):
        w_query = arrays[5]
        if can_swap(mesh, w_query.shape[1]):
            return swapped_on_device(mesh, *arrays)
        return on_device(*arrays)

    return run


def solution(mesh):
    return jax.shard_map(
        either_on_device(mesh),
        mesh=mesh,
        in_specs=(
            P(("dp", "tensor"), None),
            P("dp"),
            P(("dp", "tensor"), None),
            P(),
            P(),
            P("dp", "tensor"),
            P("tensor"),
            P("dp", "tensor"),
            P("dp", "tensor"),
            P("tensor"),
            P("tensor", "dp"),
            P(),
            P(),
            P(),
            P("dp", "tensor"),
            P("tensor"),
            P("tensor", "dp"),
            P(),
        ),
        out_specs=(
            P(("dp", "tensor"), None),
            P(("dp", "tensor"), None),
            P(),
            P(),
            P("dp", "tensor"),
            P("tensor"),
            P("dp", "tensor"),
            P("dp", "tensor"),
            P("tensor"),
            P("tensor", "dp"),
            P(),
            P(),
            P(),
            P("dp", "tensor"),
            P("tensor"),
            P("tensor", "dp"),
            P(),
        ),
        check_vma=False,
    )
```

```python
import functools
import math

import jax
import jax.numpy as jnp
from jax import lax
from jax.experimental import pallas as pl
from jax.experimental.pallas import tpu as pltpu
from jax.sharding import PartitionSpec as P

HDIM = 128
QBLK = 768


EPS = 1e-05
NEG = -1e30


def layer_norm(values, norm_gain, norm_shift):
    row_mean = jnp.mean(values, axis=-1, keepdims=True)
    centred = values - row_mean
    row_var = jnp.mean(centred * centred, axis=-1, keepdims=True)
    return centred * lax.rsqrt(row_var + EPS) * norm_gain + norm_shift


def gelu_exact(values):
    return jax.nn.gelu(values, approximate=False)


def row_dot(left_side, right_side):
    return jnp.dot(left_side, right_side, preferred_element_type=jnp.float32)


def left_dot(left_side, right_side):
    return lax.dot_general(
        left_side, right_side, (((0,), (0,)), ((), ())), preferred_element_type=jnp.float32
    )


def back_dot(left_side, right_side):
    return lax.dot_general(
        left_side, right_side, (((1,), (1,)), ((), ())), preferred_element_type=jnp.float32
    )


def visible(segments, first_row, row_count, key_end):
    query_pos = first_row + jnp.arange(row_count)
    key_pos = jnp.arange(key_end)
    seg_query = segments[first_row : first_row + row_count]
    seg_key = segments[:key_end]
    causal = key_pos[None, :] <= query_pos[:, None]
    shared = (seg_key[None, :] == seg_query[:, None]) | (seg_key[None, :] == 0)
    return causal & shared


def attend_block(queries, key_rows, value_rows, allowed):
    scores = jnp.einsum("qhd,khd->hqk", queries, key_rows, preferred_element_type=jnp.float32)
    scores = jnp.where(allowed[None], scores, NEG)
    row_top = jnp.max(scores, axis=-1, keepdims=True)
    raised = jnp.exp(scores - row_top)
    row_total = jnp.sum(raised, axis=-1, keepdims=True)
    weights = raised / row_total
    mixed = jnp.einsum(
        "hqk,khd->qhd", weights.astype(jnp.bfloat16), value_rows, preferred_element_type=jnp.float32
    )
    return (mixed.astype(jnp.bfloat16), row_top + jnp.log(row_total))


def attend_back(queries, key_rows, value_rows, grad_out, log_total, allowed):
    scores = jnp.einsum("qhd,khd->hqk", queries, key_rows, preferred_element_type=jnp.float32)
    weights = jnp.where(allowed[None], jnp.exp(scores - log_total), 0.0)
    grad_weights = jnp.einsum(
        "qhd,khd->hqk", grad_out, value_rows, preferred_element_type=jnp.float32
    )
    inner = jnp.sum(weights * grad_weights, axis=-1, keepdims=True)
    grad_scores = (weights * (grad_weights - inner)).astype(jnp.bfloat16)
    grad_query = jnp.einsum(
        "hqk,khd->qhd", grad_scores, key_rows, preferred_element_type=jnp.float32
    )
    grad_key = jnp.einsum("hqk,qhd->khd", grad_scores, queries, preferred_element_type=jnp.float32)
    grad_value = jnp.einsum(
        "hqk,qhd->khd", weights.astype(jnp.bfloat16), grad_out, preferred_element_type=jnp.float32
    )
    return (grad_query, grad_key, grad_value)


def on_device(
    tokens,
    segments,
    cotangent,
    ln1_gain,
    ln1_shift,
    w_query,
    b_query,
    w_key,
    w_value,
    b_value,
    w_out,
    b_out,
    ln2_gain,
    ln2_shift,
    w_up,
    b_up,
    w_down,
    b_down,
):
    score_scale = 1.0 / math.sqrt(HDIM)
    full_query, full_key, full_value, full_out, full_up, full_down = (
        lax.all_gather(w_query, "dp", axis=0, tiled=True),
        lax.all_gather(w_key, "dp", axis=0, tiled=True),
        lax.all_gather(w_value, "dp", axis=0, tiled=True),
        lax.all_gather(w_out, "dp", axis=1, tiled=True),
        lax.all_gather(w_up, "dp", axis=0, tiled=True),
        lax.all_gather(w_down, "dp", axis=1, tiled=True),
    )
    group_len = segments.shape[0]
    head_cols = full_query.shape[1]
    heads_here = head_cols // HDIM
    block_count = group_len // QBLK
    inputs = tokens.astype(jnp.float32)
    normed_one, norm_one_back = jax.vjp(
        layer_norm, inputs, ln1_gain.astype(jnp.float32), ln1_shift.astype(jnp.float32)
    )
    h_one = normed_one.astype(jnp.bfloat16)
    h_one_full = lax.all_gather(h_one, "tensor", axis=0, tiled=True)
    w_qkv = jnp.concatenate([full_query, full_key, full_value], axis=1)
    w_kv = w_qkv[:, head_cols:]
    projected = row_dot(h_one_full, w_qkv)
    queries = ((projected[:, :head_cols] + b_query.astype(jnp.float32)) * score_scale).astype(
        jnp.bfloat16
    )
    key_rows = projected[:, head_cols : 2 * head_cols].astype(jnp.bfloat16)
    value_rows = (projected[:, 2 * head_cols :] + b_value.astype(jnp.float32)).astype(jnp.bfloat16)
    query3 = queries.reshape(group_len, heads_here, HDIM)
    key3 = key_rows.reshape(group_len, heads_here, HDIM)
    value3 = value_rows.reshape(group_len, heads_here, HDIM)
    pieces = []
    totals = []
    for block in range(block_count):
        first_row = block * QBLK
        key_end = first_row + QBLK
        allowed = visible(segments, first_row, QBLK, key_end)
        mixed_block, log_total = attend_block(
            query3[first_row:key_end], key3[:key_end], value3[:key_end], allowed
        )
        pieces.append(mixed_block)
        totals.append(log_total)
    attended = jnp.concatenate(pieces, axis=0).reshape(group_len, head_cols)
    resid = (
        inputs
        + lax.psum_scatter(row_dot(attended, full_out), "tensor", scatter_dimension=0, tiled=True)
        + b_out.astype(jnp.float32)
    )
    normed_two, norm_two_back = jax.vjp(
        layer_norm, resid, ln2_gain.astype(jnp.float32), ln2_shift.astype(jnp.float32)
    )
    h_two = normed_two.astype(jnp.bfloat16)
    h_two_full = lax.all_gather(h_two, "tensor", axis=0, tiled=True)
    pre_act = row_dot(h_two_full, full_up) + b_up.astype(jnp.float32)
    activated, gelu_back = jax.vjp(gelu_exact, pre_act)
    act_low = activated.astype(jnp.bfloat16)
    output = (
        resid
        + lax.psum_scatter(
            row_dot(act_low, full_down).astype(jnp.bfloat16),
            "tensor",
            scatter_dimension=0,
            tiled=True,
        ).astype(jnp.float32)
        + b_down.astype(jnp.float32)
    ).astype(jnp.bfloat16)
    grad_y = cotangent.astype(jnp.float32)
    grad_y_full = lax.all_gather(cotangent, "tensor", axis=0, tiled=True)
    grad_down = left_dot(act_low, grad_y_full)
    grad_act = back_dot(grad_y_full, full_down)
    grad_pre = gelu_back(grad_act)[0].astype(jnp.bfloat16)
    grad_bias_up = jnp.sum(grad_pre.astype(jnp.float32), axis=0)
    grad_up = left_dot(h_two_full, grad_pre)
    grad_h_two = lax.psum_scatter(
        back_dot(grad_pre, full_up), "tensor", scatter_dimension=0, tiled=True
    )
    grad_resid_norm, grad_gain_two, grad_shift_two = norm_two_back(grad_h_two)
    grad_resid = grad_y + grad_resid_norm
    grad_mix = grad_resid.astype(jnp.bfloat16)
    grad_bias_out = jnp.sum(grad_mix.astype(jnp.float32), axis=0)
    grad_bias_down = jnp.sum(grad_y, axis=0)
    grad_mix_full = lax.all_gather(grad_mix, "tensor", axis=0, tiled=True)
    grad_out_w = left_dot(attended, grad_mix_full)
    grad_att = (
        back_dot(grad_mix_full, full_out).astype(jnp.bfloat16).reshape(group_len, heads_here, HDIM)
    )
    grad_key_sum = jnp.zeros((group_len, heads_here, HDIM), jnp.float32)
    grad_value_sum = jnp.zeros((group_len, heads_here, HDIM), jnp.float32)
    query_grads = []
    for block in range(block_count):
        first_row = block * QBLK
        key_end = first_row + QBLK
        allowed = visible(segments, first_row, QBLK, key_end)
        grad_q_block, grad_k_part, grad_v_part = attend_back(
            query3[first_row:key_end],
            key3[:key_end],
            value3[:key_end],
            grad_att[first_row:key_end],
            totals[block],
            allowed,
        )
        query_grads.append(grad_q_block.astype(jnp.bfloat16))
        grad_key_sum = grad_key_sum.at[:key_end].add(grad_k_part)
        grad_value_sum = grad_value_sum.at[:key_end].add(grad_v_part)
    grad_q = jnp.concatenate(query_grads, axis=0).reshape(group_len, head_cols)
    grad_k = grad_key_sum.reshape(group_len, head_cols).astype(jnp.bfloat16)
    grad_v = grad_value_sum.reshape(group_len, head_cols).astype(jnp.bfloat16)
    grad_qkv = jnp.concatenate([grad_q, grad_k, grad_v], axis=1)
    grad_qkv_w = left_dot(h_one_full, grad_qkv)
    grad_wq = grad_qkv_w[:, :head_cols] * score_scale
    grad_wk = grad_qkv_w[:, head_cols : 2 * head_cols]
    grad_wv = grad_qkv_w[:, 2 * head_cols :]
    grad_bias_query = jnp.sum(grad_q.astype(jnp.float32), axis=0) * score_scale
    grad_bias_value = jnp.sum(grad_v.astype(jnp.float32), axis=0)
    grad_h_one = lax.psum_scatter(
        (
            back_dot(grad_qkv[:, :head_cols], full_query) * score_scale
            + back_dot(grad_qkv[:, head_cols:], w_kv)
        ).astype(jnp.bfloat16),
        "tensor",
        scatter_dimension=0,
        tiled=True,
    ).astype(jnp.float32)
    grad_in_norm, grad_gain_one, grad_shift_one = norm_one_back(grad_h_one)
    input_grad = (grad_resid + grad_in_norm).astype(jnp.bfloat16)
    sent_query, sent_key, sent_value, sent_out, sent_up, sent_down = (
        lax.psum_scatter(
            grad_wq.astype(jnp.bfloat16), "dp", scatter_dimension=0, tiled=True
        ).astype(jnp.float32),
        lax.psum_scatter(
            grad_wk.astype(jnp.bfloat16), "dp", scatter_dimension=0, tiled=True
        ).astype(jnp.float32),
        lax.psum_scatter(
            grad_wv.astype(jnp.bfloat16), "dp", scatter_dimension=0, tiled=True
        ).astype(jnp.float32),
        lax.psum_scatter(
            grad_out_w.astype(jnp.bfloat16), "dp", scatter_dimension=1, tiled=True
        ).astype(jnp.float32),
        lax.psum_scatter(
            grad_up.astype(jnp.bfloat16), "dp", scatter_dimension=0, tiled=True
        ).astype(jnp.float32),
        lax.psum_scatter(
            grad_down.astype(jnp.bfloat16), "dp", scatter_dimension=1, tiled=True
        ).astype(jnp.float32),
    )
    summed_query, summed_value, summed_up = lax.psum(
        (grad_bias_query, grad_bias_value, grad_bias_up), "dp"
    )
    gain_one_sum, shift_one_sum, gain_two_sum, shift_two_sum, bias_out_sum, bias_down_sum = (
        lax.psum(
            (
                grad_gain_one,
                grad_shift_one,
                grad_gain_two,
                grad_shift_two,
                grad_bias_out,
                grad_bias_down,
            ),
            ("dp", "tensor"),
        )
    )
    return (
        output,
        input_grad,
        gain_one_sum,
        shift_one_sum,
        sent_query,
        summed_query,
        sent_key,
        sent_value,
        summed_value,
        sent_out,
        bias_out_sum,
        gain_two_sum,
        shift_two_sum,
        sent_up,
        summed_up,
        sent_down,
        bias_down_sum,
    )


def attend_rows(perm_ref, qkv_ref, seg_col_ref, seg_row_ref, out_ref, log_ref, *, count, rows):
    for at in range(count):
        place = pl.multiple_of(perm_ref[at] * rows, rows)
        query = qkv_ref[pl.ds(place, rows), :HDIM]
        scores = []
        for key_at in range(at + 1):
            key_place = pl.multiple_of(perm_ref[key_at] * rows, rows)
            score = back_dot(query, qkv_ref[pl.ds(key_place, rows), HDIM : 2 * HDIM])
            allowed = block_allowed(seg_col_ref, seg_row_ref, at, key_at, rows)
            scores.append(jnp.where(allowed, score, NEG))
        row_top = functools.reduce(
            jnp.maximum, [jnp.max(score, axis=-1, keepdims=True) for score in scores]
        )
        raised = [jnp.exp(score - row_top) for score in scores]
        row_total = sum(jnp.sum(item, axis=-1, keepdims=True) for item in raised)
        inverse = 1.0 / row_total
        mixed = jnp.zeros((rows, HDIM), jnp.float32)
        for key_at in range(at + 1):
            key_place = pl.multiple_of(perm_ref[key_at] * rows, rows)
            mixed = mixed + row_dot(
                (raised[key_at] * inverse).astype(jnp.bfloat16),
                qkv_ref[pl.ds(key_place, rows), 2 * HDIM :],
            )
        out_ref[pl.ds(place, rows), :] = mixed.astype(jnp.bfloat16)
        log_ref[0, at * rows : (at + 1) * rows, :] = row_top + jnp.log(row_total)


def block_allowed(seg_col_ref, seg_row_ref, at, key_at, rows):
    seg_query = seg_col_ref[at * rows : (at + 1) * rows, :]
    seg_key = seg_row_ref[:, key_at * rows : (key_at + 1) * rows]
    shared = (seg_key == seg_query) | (seg_key == 0)
    if at > key_at:
        return shared
    query_pos = lax.broadcasted_iota(jnp.int32, (rows, rows), 0)
    key_pos = lax.broadcasted_iota(jnp.int32, (rows, rows), 1)
    return shared & (key_pos <= query_pos)


def attend_rows_back(
    perm_ref, qkv_ref, grad_ref, log_ref, seg_col_ref, seg_row_ref, out_ref, sum_ref,
    weight_ref, slope_ref, key_sum_ref, value_sum_ref, *, count, rows, score_scale,
):
    query_total = jnp.zeros((1, HDIM), jnp.float32)
    for at in range(count):
        place = pl.multiple_of(perm_ref[at] * rows, rows)
        query = qkv_ref[pl.ds(place, rows), :HDIM]
        grad_out = grad_ref[pl.ds(place, rows), :]
        log_total = log_ref[0, at * rows : (at + 1) * rows, :]
        inner = jnp.zeros((rows, 1), jnp.float32)
        for key_at in range(at + 1):
            key_place = pl.multiple_of(perm_ref[key_at] * rows, rows)
            span = slice(key_at * rows, (key_at + 1) * rows)
            score = back_dot(query, qkv_ref[pl.ds(key_place, rows), HDIM : 2 * HDIM])
            allowed = block_allowed(seg_col_ref, seg_row_ref, at, key_at, rows)
            weight = jnp.exp(jnp.where(allowed, score - log_total, NEG))
            slope = back_dot(grad_out, qkv_ref[pl.ds(key_place, rows), 2 * HDIM :])
            inner = inner + jnp.sum(weight * slope, axis=-1, keepdims=True)
            weight_ref[:, span] = weight
            slope_ref[:, span] = slope
        grad_query = jnp.zeros((rows, HDIM), jnp.float32)
        for key_at in range(at + 1):
            key_place = pl.multiple_of(perm_ref[key_at] * rows, rows)
            span = slice(key_at * rows, (key_at + 1) * rows)
            weight = weight_ref[:, span]
            grad_score = (weight * (slope_ref[:, span] - inner)).astype(jnp.bfloat16)
            grad_query = grad_query + row_dot(
                grad_score, qkv_ref[pl.ds(key_place, rows), HDIM : 2 * HDIM]
            )
            key_part = left_dot(grad_score, query)
            value_part = left_dot(weight.astype(jnp.bfloat16), grad_out)
            if at > key_at:
                key_part = key_part + key_sum_ref[span, :]
                value_part = value_part + value_sum_ref[span, :]
            key_sum_ref[span, :] = key_part
            value_sum_ref[span, :] = value_part
        grad_low = (grad_query * score_scale).astype(jnp.bfloat16)
        out_ref[pl.ds(place, rows), :HDIM] = grad_low
        query_total = query_total + jnp.sum(grad_low.astype(jnp.float32), axis=0, keepdims=True)
    value_total = jnp.zeros((1, HDIM), jnp.float32)
    for at in range(count):
        place = pl.multiple_of(perm_ref[at] * rows, rows)
        span = slice(at * rows, (at + 1) * rows)
        out_ref[pl.ds(place, rows), HDIM : 2 * HDIM] = key_sum_ref[span, :].astype(jnp.bfloat16)
        value_low = value_sum_ref[span, :].astype(jnp.bfloat16)
        out_ref[pl.ds(place, rows), 2 * HDIM :] = value_low
        value_total = value_total + jnp.sum(value_low.astype(jnp.float32), axis=0, keepdims=True)
    sum_ref[0, :, :HDIM] = jnp.broadcast_to(query_total, (8, HDIM))
    sum_ref[0, :, HDIM:] = jnp.broadcast_to(value_total, (8, HDIM))


def attention(perm, qkv, segments):
    length, heads, count = qkv.shape[0], qkv.shape[1] // (3 * HDIM), perm.shape[0]
    pairs = length * length // 2 * HDIM * heads
    return pl.pallas_call(
        functools.partial(attend_rows, count=count, rows=length // count),
        out_shape=(
            jax.ShapeDtypeStruct((length, heads * HDIM), jnp.bfloat16),
            jax.ShapeDtypeStruct((heads, length, 1), jnp.float32),
        ),
        grid_spec=pltpu.PrefetchScalarGridSpec(
            num_scalar_prefetch=1,
            grid=(heads,),
            in_specs=[
                pl.BlockSpec((length, 3 * HDIM), lambda head, perm: (0, head)),
                pl.BlockSpec((length, 1), lambda head, perm: (0, 0)),
                pl.BlockSpec((1, length), lambda head, perm: (0, 0)),
            ],
            out_specs=[
                pl.BlockSpec((length, HDIM), lambda head, perm: (0, head)),
                pl.BlockSpec((1, length, 1), lambda head, perm: (head, 0, 0)),
            ],
        ),
        cost_estimate=pl.CostEstimate(
            flops=4 * pairs, bytes_accessed=8 * length * heads * HDIM, transcendentals=pairs // HDIM
        ),
        name="attention",
    )(perm, qkv, segments.reshape(length, 1), segments.reshape(1, length))


def attention_back(perm, qkv, grad_att, log_total, segments, score_scale):
    length, heads, count = qkv.shape[0], qkv.shape[1] // (3 * HDIM), perm.shape[0]
    rows = length // count
    pairs = length * length // 2 * HDIM * heads
    return pl.pallas_call(
        functools.partial(attend_rows_back, count=count, rows=rows, score_scale=score_scale),
        out_shape=(
            jax.ShapeDtypeStruct(qkv.shape, jnp.bfloat16),
            jax.ShapeDtypeStruct((heads, 8, 2 * HDIM), jnp.float32),
        ),
        grid_spec=pltpu.PrefetchScalarGridSpec(
            num_scalar_prefetch=1,
            grid=(heads,),
            in_specs=[
                pl.BlockSpec((length, 3 * HDIM), lambda head, perm: (0, head)),
                pl.BlockSpec((length, HDIM), lambda head, perm: (0, head)),
                pl.BlockSpec((1, length, 1), lambda head, perm: (head, 0, 0)),
                pl.BlockSpec((length, 1), lambda head, perm: (0, 0)),
                pl.BlockSpec((1, length), lambda head, perm: (0, 0)),
            ],
            out_specs=[
                pl.BlockSpec((length, 3 * HDIM), lambda head, perm: (0, head)),
                pl.BlockSpec((1, 8, 2 * HDIM), lambda head, perm: (head, 0, 0)),
            ],
            scratch_shapes=[
                pltpu.VMEM((rows, length), jnp.float32),
                pltpu.VMEM((rows, length), jnp.float32),
                pltpu.VMEM((length, HDIM), jnp.float32),
                pltpu.VMEM((length, HDIM), jnp.float32),
            ],
        ),
        cost_estimate=pl.CostEstimate(
            flops=10 * pairs, bytes_accessed=16 * length * heads * HDIM, transcendentals=pairs // HDIM
        ),
        name="attention_back",
    )(perm, qkv, grad_att, log_total, segments.reshape(length, 1), segments.reshape(1, length))


def power_of_two(count):
    return count > 0 and count & (count - 1) == 0


def mirrored(value, count):
    bits = count.bit_length() - 1
    out = 0 * value
    for bit in range(bits):
        out = out + ((value >> bit) & 1) * (1 << (bits - 1 - bit))
    return out


class Links:
    def __init__(self, mesh):
        self.cols = mesh.shape["tensor"]
        self.ranks = self.cols
        self.halves = mesh.shape["dp"] // self.ranks
        dp_index = lax.axis_index("dp")
        self.half = dp_index // self.ranks
        self.rank = dp_index % self.ranks
        self.col = lax.axis_index("tensor")
        self.quarter = mirrored(self.rank, self.ranks)

    def moved(self, values, target):
        pairs = []
        for half in range(self.halves):
            for rank in range(self.ranks):
                for col in range(self.cols):
                    to_half, to_rank, to_col = target(half, rank, col)
                    pairs.append(
                        (
                            (half * self.ranks + rank) * self.cols + col,
                            (to_half * self.ranks + to_rank) * self.cols + to_col,
                        )
                    )
        return lax.ppermute(values, ("dp", "tensor"), pairs)

    def swap(self, values):
        return self.moved(
            values, lambda half, rank, col: (half, mirrored(col, self.cols), mirrored(rank, self.ranks))
        )

    def rank_pair(self, values, bit):
        return self.moved(values, lambda half, rank, col: (half, rank ^ bit, col))

    def half_pair(self, values, bit):
        return self.moved(values, lambda half, rank, col: (half ^ bit, rank, col))

    def col_pair(self, values, bit):
        return self.moved(values, lambda half, rank, col: (half, rank, col ^ bit))

    def gather_cols(self, values):
        rows = []
        for at in range(self.cols):
            got = values if at == 0 else self.col_pair(values, at)
            place = (jnp.arange(self.cols) == (self.col ^ at)).astype(values.dtype)
            rows.append(place[:, None] * got[None, :])
        return sum(rows)

    def total(self, values):
        for pair, count in (
            (self.rank_pair, self.ranks),
            (self.half_pair, self.halves),
            (self.col_pair, self.cols),
        ):
            bit = 1
            while bit < count:
                values = values + pair(values, bit)
                bit *= 2
        return values

    def rank_bits(self):
        return [1 << place for place in range(self.ranks.bit_length() - 1)]

    def gather_rows(self, piece):
        pieces = {0: piece}
        for bit in reversed(self.rank_bits()):
            for at in list(pieces):
                pieces[at | bit] = self.rank_pair(pieces[at], bit)
        return [pieces[at] for at in range(self.ranks)]

    def scatter_rows(self, pieces):
        sums = dict(enumerate(pieces))
        for bit in self.rank_bits():
            for at in [item for item in sums if item & bit]:
                arrived = self.rank_pair(sums.pop(at).astype(jnp.bfloat16), bit)
                sums[at ^ bit] = sums[at ^ bit] + arrived.astype(jnp.float32)
        return sums[0]

    def half_order(self, values, axis):
        if self.halves == 1:
            return values
        width = values.shape[axis] // self.halves
        return jnp.concatenate(
            [
                lax.dynamic_slice_in_dim(values, (self.half ^ at) * width, width, axis)
                for at in range(self.halves)
            ],
            axis=axis,
        )

    def places(self):
        return jnp.stack(
            [mirrored(at ^ self.quarter, self.ranks) for at in range(self.ranks)]
        ).astype(jnp.int32)

    def row_order(self, pieces):
        stacked = jnp.concatenate(pieces, axis=0)
        rows = pieces[0].shape[0]
        return jnp.concatenate(
            [
                lax.dynamic_slice_in_dim(
                    stacked, mirrored(at ^ self.quarter, self.ranks) * rows, rows, 0
                )
                for at in range(self.ranks)
            ],
            axis=0,
        )

    def piece_order(self, values):
        rows = values.shape[0] // self.ranks
        return [
            lax.dynamic_slice_in_dim(
                values, (self.quarter ^ mirrored(at, self.ranks)) * rows, rows, 0
            )
            for at in range(self.ranks)
        ]

    def rank_groups(self):
        return [
            [half * self.ranks + rank for rank in range(self.ranks)] for half in range(self.halves)
        ]

    def spread(self, shard, hidden_axis):
        other = 1 - hidden_axis
        part = lax.all_to_all(
            shard, "dp", hidden_axis, other, axis_index_groups=self.rank_groups(), tiled=True
        )
        part = lax.all_gather(part, "tensor", axis=hidden_axis, tiled=True)
        parts = {0: part}
        bit = self.halves // 2
        while bit:
            for at in list(parts):
                parts[at | bit] = self.half_pair(parts[at], bit)
            bit //= 2
        return jnp.concatenate([parts[at] for at in range(self.halves)], axis=other)

    def collect(self, grad, hidden_axis):
        other = 1 - hidden_axis
        width = grad.shape[other] // self.halves
        sums = {
            at: lax.slice_in_dim(grad, at * width, (at + 1) * width, axis=other)
            for at in range(self.halves)
        }
        bit = 1
        while bit < self.halves:
            for at in [item for item in sums if item & bit]:
                arrived = self.half_pair(sums.pop(at).astype(jnp.bfloat16), bit)
                sums[at ^ bit] = sums[at ^ bit] + arrived.astype(jnp.float32)
            bit *= 2
        part = lax.psum_scatter(
            sums[0].astype(jnp.bfloat16), "tensor", scatter_dimension=hidden_axis, tiled=True
        )
        return lax.all_to_all(
            part, "dp", other, hidden_axis, axis_index_groups=self.rank_groups(), tiled=True
        ).astype(jnp.float32)

    def rank_part(self, values):
        width = values.shape[0] // self.ranks
        return lax.dynamic_slice_in_dim(values, self.rank * width, width, 0)

    def rank_slots(self, values):
        mine = (jnp.arange(self.ranks) == self.rank).astype(values.dtype)
        blocks = values.reshape(self.cols, 1, -1)
        return (blocks * mine[None, :, None]).reshape(-1)


def swapped_on_device(
    mesh,
    tokens,
    segments,
    cotangent,
    ln1_gain,
    ln1_shift,
    w_query,
    b_query,
    w_key,
    w_value,
    b_value,
    w_out,
    b_out,
    ln2_gain,
    ln2_shift,
    w_up,
    b_up,
    w_down,
    b_down,
):
    links = Links(mesh)
    ranks, cols = links.ranks, links.cols
    score_scale = 1.0 / math.sqrt(HDIM)
    group_len = segments.shape[0]
    head_cols = w_query.shape[1]
    heads_here = head_cols // HDIM
    sub_cols = head_cols // ranks
    block_count = group_len // QBLK
    f32 = jnp.float32
    low = jnp.bfloat16

    tokens = links.half_order(links.swap(tokens), 1)
    segments = links.swap(segments)

    w_qkv_shard = jnp.concatenate(
        [item.reshape(-1, ranks, sub_cols) for item in (w_query, w_key, w_value)], axis=2
    ).reshape(w_query.shape[0], -1)
    biases = jnp.concatenate([links.rank_part(item) for item in (b_query, b_value, b_up)])
    biases = links.gather_cols(biases.astype(f32))
    bias_query = biases[:, :sub_cols].reshape(-1)
    bias_value = biases[:, sub_cols : 2 * sub_cols].reshape(-1)
    bias_up = biases[:, 2 * sub_cols :].reshape(-1)
    full_qkv = links.spread(w_qkv_shard, 1)
    full_out = links.spread(w_out, 0)
    full_up = links.spread(w_up, 1)
    full_down = links.spread(w_down, 0)

    gain_one, shift_one, gain_two, shift_two, out_bias, down_bias = (
        links.half_order(item.astype(f32), 0)
        for item in (ln1_gain, ln1_shift, ln2_gain, ln2_shift, b_out, b_down)
    )

    inputs = tokens.astype(f32)
    normed_one, norm_one_back = jax.vjp(layer_norm, inputs, gain_one, shift_one)
    h_one_pieces = links.gather_rows(normed_one.astype(low))
    blocks = (heads_here, 1, HDIM)
    no_bias = jnp.zeros(blocks, f32)
    qkv_bias = jnp.concatenate(
        [bias_query.reshape(blocks), no_bias, bias_value.reshape(blocks)], axis=1
    ).reshape(-1)
    qkv_scale = jnp.concatenate(
        [jnp.full(blocks, score_scale, f32), jnp.ones((heads_here, 2, HDIM), f32)], axis=1
    ).reshape(-1)
    qkv = jnp.concatenate(
        [((row_dot(piece, full_qkv) + qkv_bias) * qkv_scale).astype(low) for piece in h_one_pieces],
        axis=0,
    )
    places = links.places()
    attended, log_total = attention(places, qkv, segments)
    rows = tokens.shape[0]
    attended_pieces = [attended[at * rows : (at + 1) * rows] for at in range(ranks)]
    resid = (
        inputs
        + links.scatter_rows([row_dot(piece, full_out) for piece in attended_pieces])
        + out_bias
    )
    normed_two, norm_two_back = jax.vjp(layer_norm, resid, gain_two, shift_two)
    h_two = jnp.concatenate(links.gather_rows(normed_two.astype(low)), axis=0)
    pre_act = row_dot(h_two, full_up) + bias_up
    activated, gelu_back = jax.vjp(gelu_exact, pre_act)
    act_low = activated.astype(low)
    output = (
        resid
        + links.scatter_rows(
            [row_dot(act_low[at * rows : (at + 1) * rows], full_down) for at in range(ranks)]
        )
        + down_bias
    ).astype(low)
    output = links.swap(links.half_order(output, 1))

    grad_y_low = links.half_order(links.swap(cotangent), 1)
    grad_y = grad_y_low.astype(f32)
    grad_y_full = jnp.concatenate(links.gather_rows(grad_y_low), axis=0)
    sent_down = links.collect(left_dot(act_low, grad_y_full), 0)
    grad_act = back_dot(grad_y_full, full_down)
    grad_pre = gelu_back(grad_act)[0].astype(low)
    grad_bias_up = jnp.sum(grad_pre.astype(f32), axis=0)
    sent_up = links.collect(left_dot(h_two, grad_pre), 1)
    grad_h_two = links.scatter_rows(
        [back_dot(grad_pre[at * rows : (at + 1) * rows], full_up) for at in range(ranks)]
    )
    grad_resid_norm, grad_gain_two, grad_shift_two = norm_two_back(grad_h_two)
    grad_resid = grad_y + grad_resid_norm
    grad_mix = grad_resid.astype(low)
    grad_bias_out = jnp.sum(grad_mix.astype(f32), axis=0)
    grad_bias_down = jnp.sum(grad_y, axis=0)
    grad_mix_pieces = links.gather_rows(grad_mix)
    grad_mix_full = jnp.concatenate(grad_mix_pieces, axis=0)
    sent_out = links.collect(left_dot(attended, grad_mix_full), 0)
    grad_att = jnp.concatenate(
        [back_dot(piece, full_out).astype(low) for piece in grad_mix_pieces], axis=0
    )
    grad_qkv, bias_sums = attention_back(places, qkv, grad_att, log_total, segments, score_scale)
    grad_bias_query = bias_sums[:, 0, :HDIM].reshape(-1)
    grad_bias_value = bias_sums[:, 0, HDIM:].reshape(-1)
    grad_w_qkv = left_dot(jnp.concatenate(h_one_pieces, axis=0), grad_qkv)
    sent_qkv = links.collect(grad_w_qkv, 1).reshape(w_query.shape[0], ranks, 3, sub_cols)
    sent_query, sent_key, sent_value = (
        sent_qkv[:, :, at].reshape(w_query.shape) for at in range(3)
    )
    grad_h_one = links.scatter_rows(
        [back_dot(grad_qkv[at * rows : (at + 1) * rows], full_qkv) for at in range(ranks)]
    )
    grad_in_norm, grad_gain_one, grad_shift_one = norm_one_back(grad_h_one)
    input_grad = (grad_resid + grad_in_norm).astype(low)
    input_grad = links.swap(links.half_order(input_grad, 1))

    def my_block(values):
        width = values.shape[0] // cols
        return lax.dynamic_slice_in_dim(values, links.col * width, width, 0)

    def summed(*vectors):
        packed = links.total(jnp.concatenate(vectors).reshape(-1, 128)).reshape(-1)
        ends = [sum(item.size for item in vectors[: at + 1]) for at in range(len(vectors))]
        return [packed[end - item.size : end] for item, end in zip(vectors, ends)]

    early = summed(
        links.rank_slots(grad_bias_up),
        links.half_order(grad_gain_two, 0),
        links.half_order(grad_shift_two, 0),
        links.half_order(grad_bias_out, 0),
        links.half_order(grad_bias_down, 0),
    )
    late = summed(
        links.rank_slots(grad_bias_query),
        links.rank_slots(grad_bias_value),
        links.half_order(grad_gain_one, 0),
        links.half_order(grad_shift_one, 0),
    )
    return (
        output,
        input_grad,
        late[2],
        late[3],
        sent_query,
        my_block(late[0]),
        sent_key,
        sent_value,
        my_block(late[1]),
        sent_out,
        early[3],
        early[1],
        early[2],
        sent_up,
        my_block(early[0]),
        sent_down,
        early[4],
    )


def can_swap(mesh, head_cols):
    ranks = mesh.shape["tensor"]
    dp_size = mesh.shape["dp"]
    if dp_size % ranks or not power_of_two(ranks) or not power_of_two(dp_size // ranks):
        return False
    return head_cols % (ranks * HDIM) == 0


def either_on_device(mesh):
    def run(*arrays):
        w_query = arrays[5]
        if can_swap(mesh, w_query.shape[1]):
            return swapped_on_device(mesh, *arrays)
        return on_device(*arrays)

    return run


def solution(mesh):
    return jax.shard_map(
        either_on_device(mesh),
        mesh=mesh,
        in_specs=(
            P(("dp", "tensor"), None),
            P("dp"),
            P(("dp", "tensor"), None),
            P(),
            P(),
            P("dp", "tensor"),
            P("tensor"),
            P("dp", "tensor"),
            P("dp", "tensor"),
            P("tensor"),
            P("tensor", "dp"),
            P(),
            P(),
            P(),
            P("dp", "tensor"),
            P("tensor"),
            P("tensor", "dp"),
            P(),
        ),
        out_specs=(
            P(("dp", "tensor"), None),
            P(("dp", "tensor"), None),
            P(),
            P(),
            P("dp", "tensor"),
            P("tensor"),
            P("dp", "tensor"),
            P("dp", "tensor"),
            P("tensor"),
            P("tensor", "dp"),
            P(),
            P(),
            P(),
            P("dp", "tensor"),
            P("tensor"),
            P("tensor", "dp"),
            P(),
        ),
        check_vma=False,
    )
```

```python
import functools
import math

import jax
import jax.numpy as jnp
from jax import lax
from jax.experimental import pallas as pl
from jax.experimental.pallas import tpu as pltpu
from jax.sharding import PartitionSpec as P

HDIM = 128
QBLK = 768


EPS = 1e-05
NEG = -1e30


def layer_norm(values, norm_gain, norm_shift):
    row_mean = jnp.mean(values, axis=-1, keepdims=True)
    centred = values - row_mean
    row_var = jnp.mean(centred * centred, axis=-1, keepdims=True)
    return centred * lax.rsqrt(row_var + EPS) * norm_gain + norm_shift


def gelu_exact(values):
    return jax.nn.gelu(values, approximate=False)


def row_dot(left_side, right_side):
    return jnp.dot(left_side, right_side, preferred_element_type=jnp.float32)


def left_dot(left_side, right_side):
    return lax.dot_general(
        left_side, right_side, (((0,), (0,)), ((), ())), preferred_element_type=jnp.float32
    )


def back_dot(left_side, right_side):
    return lax.dot_general(
        left_side, right_side, (((1,), (1,)), ((), ())), preferred_element_type=jnp.float32
    )


def visible(segments, first_row, row_count, key_end):
    query_pos = first_row + jnp.arange(row_count)
    key_pos = jnp.arange(key_end)
    seg_query = segments[first_row : first_row + row_count]
    seg_key = segments[:key_end]
    causal = key_pos[None, :] <= query_pos[:, None]
    shared = (seg_key[None, :] == seg_query[:, None]) | (seg_key[None, :] == 0)
    return causal & shared


def attend_block(queries, key_rows, value_rows, allowed):
    scores = jnp.einsum("qhd,khd->hqk", queries, key_rows, preferred_element_type=jnp.float32)
    scores = jnp.where(allowed[None], scores, NEG)
    row_top = jnp.max(scores, axis=-1, keepdims=True)
    raised = jnp.exp(scores - row_top)
    row_total = jnp.sum(raised, axis=-1, keepdims=True)
    weights = raised / row_total
    mixed = jnp.einsum(
        "hqk,khd->qhd", weights.astype(jnp.bfloat16), value_rows, preferred_element_type=jnp.float32
    )
    return (mixed.astype(jnp.bfloat16), row_top + jnp.log(row_total))


def attend_back(queries, key_rows, value_rows, grad_out, log_total, allowed):
    scores = jnp.einsum("qhd,khd->hqk", queries, key_rows, preferred_element_type=jnp.float32)
    weights = jnp.where(allowed[None], jnp.exp(scores - log_total), 0.0)
    grad_weights = jnp.einsum(
        "qhd,khd->hqk", grad_out, value_rows, preferred_element_type=jnp.float32
    )
    inner = jnp.sum(weights * grad_weights, axis=-1, keepdims=True)
    grad_scores = (weights * (grad_weights - inner)).astype(jnp.bfloat16)
    grad_query = jnp.einsum(
        "hqk,khd->qhd", grad_scores, key_rows, preferred_element_type=jnp.float32
    )
    grad_key = jnp.einsum("hqk,qhd->khd", grad_scores, queries, preferred_element_type=jnp.float32)
    grad_value = jnp.einsum(
        "hqk,qhd->khd", weights.astype(jnp.bfloat16), grad_out, preferred_element_type=jnp.float32
    )
    return (grad_query, grad_key, grad_value)


def on_device(
    tokens,
    segments,
    cotangent,
    ln1_gain,
    ln1_shift,
    w_query,
    b_query,
    w_key,
    w_value,
    b_value,
    w_out,
    b_out,
    ln2_gain,
    ln2_shift,
    w_up,
    b_up,
    w_down,
    b_down,
):
    score_scale = 1.0 / math.sqrt(HDIM)
    full_query, full_key, full_value, full_out, full_up, full_down = (
        lax.all_gather(w_query, "dp", axis=0, tiled=True),
        lax.all_gather(w_key, "dp", axis=0, tiled=True),
        lax.all_gather(w_value, "dp", axis=0, tiled=True),
        lax.all_gather(w_out, "dp", axis=1, tiled=True),
        lax.all_gather(w_up, "dp", axis=0, tiled=True),
        lax.all_gather(w_down, "dp", axis=1, tiled=True),
    )
    group_len = segments.shape[0]
    head_cols = full_query.shape[1]
    heads_here = head_cols // HDIM
    block_count = group_len // QBLK
    inputs = tokens.astype(jnp.float32)
    normed_one, norm_one_back = jax.vjp(
        layer_norm, inputs, ln1_gain.astype(jnp.float32), ln1_shift.astype(jnp.float32)
    )
    h_one = normed_one.astype(jnp.bfloat16)
    h_one_full = lax.all_gather(h_one, "tensor", axis=0, tiled=True)
    w_qkv = jnp.concatenate([full_query, full_key, full_value], axis=1)
    w_kv = w_qkv[:, head_cols:]
    projected = row_dot(h_one_full, w_qkv)
    queries = ((projected[:, :head_cols] + b_query.astype(jnp.float32)) * score_scale).astype(
        jnp.bfloat16
    )
    key_rows = projected[:, head_cols : 2 * head_cols].astype(jnp.bfloat16)
    value_rows = (projected[:, 2 * head_cols :] + b_value.astype(jnp.float32)).astype(jnp.bfloat16)
    query3 = queries.reshape(group_len, heads_here, HDIM)
    key3 = key_rows.reshape(group_len, heads_here, HDIM)
    value3 = value_rows.reshape(group_len, heads_here, HDIM)
    pieces = []
    totals = []
    for block in range(block_count):
        first_row = block * QBLK
        key_end = first_row + QBLK
        allowed = visible(segments, first_row, QBLK, key_end)
        mixed_block, log_total = attend_block(
            query3[first_row:key_end], key3[:key_end], value3[:key_end], allowed
        )
        pieces.append(mixed_block)
        totals.append(log_total)
    attended = jnp.concatenate(pieces, axis=0).reshape(group_len, head_cols)
    resid = (
        inputs
        + lax.psum_scatter(row_dot(attended, full_out), "tensor", scatter_dimension=0, tiled=True)
        + b_out.astype(jnp.float32)
    )
    normed_two, norm_two_back = jax.vjp(
        layer_norm, resid, ln2_gain.astype(jnp.float32), ln2_shift.astype(jnp.float32)
    )
    h_two = normed_two.astype(jnp.bfloat16)
    h_two_full = lax.all_gather(h_two, "tensor", axis=0, tiled=True)
    pre_act = row_dot(h_two_full, full_up) + b_up.astype(jnp.float32)
    activated, gelu_back = jax.vjp(gelu_exact, pre_act)
    act_low = activated.astype(jnp.bfloat16)
    output = (
        resid
        + lax.psum_scatter(
            row_dot(act_low, full_down).astype(jnp.bfloat16),
            "tensor",
            scatter_dimension=0,
            tiled=True,
        ).astype(jnp.float32)
        + b_down.astype(jnp.float32)
    ).astype(jnp.bfloat16)
    grad_y = cotangent.astype(jnp.float32)
    grad_y_full = lax.all_gather(cotangent, "tensor", axis=0, tiled=True)
    grad_down = left_dot(act_low, grad_y_full)
    grad_act = back_dot(grad_y_full, full_down)
    grad_pre = gelu_back(grad_act)[0].astype(jnp.bfloat16)
    grad_bias_up = jnp.sum(grad_pre.astype(jnp.float32), axis=0)
    grad_up = left_dot(h_two_full, grad_pre)
    grad_h_two = lax.psum_scatter(
        back_dot(grad_pre, full_up), "tensor", scatter_dimension=0, tiled=True
    )
    grad_resid_norm, grad_gain_two, grad_shift_two = norm_two_back(grad_h_two)
    grad_resid = grad_y + grad_resid_norm
    grad_mix = grad_resid.astype(jnp.bfloat16)
    grad_bias_out = jnp.sum(grad_mix.astype(jnp.float32), axis=0)
    grad_bias_down = jnp.sum(grad_y, axis=0)
    grad_mix_full = lax.all_gather(grad_mix, "tensor", axis=0, tiled=True)
    grad_out_w = left_dot(attended, grad_mix_full)
    grad_att = (
        back_dot(grad_mix_full, full_out).astype(jnp.bfloat16).reshape(group_len, heads_here, HDIM)
    )
    grad_key_sum = jnp.zeros((group_len, heads_here, HDIM), jnp.float32)
    grad_value_sum = jnp.zeros((group_len, heads_here, HDIM), jnp.float32)
    query_grads = []
    for block in range(block_count):
        first_row = block * QBLK
        key_end = first_row + QBLK
        allowed = visible(segments, first_row, QBLK, key_end)
        grad_q_block, grad_k_part, grad_v_part = attend_back(
            query3[first_row:key_end],
            key3[:key_end],
            value3[:key_end],
            grad_att[first_row:key_end],
            totals[block],
            allowed,
        )
        query_grads.append(grad_q_block.astype(jnp.bfloat16))
        grad_key_sum = grad_key_sum.at[:key_end].add(grad_k_part)
        grad_value_sum = grad_value_sum.at[:key_end].add(grad_v_part)
    grad_q = jnp.concatenate(query_grads, axis=0).reshape(group_len, head_cols)
    grad_k = grad_key_sum.reshape(group_len, head_cols).astype(jnp.bfloat16)
    grad_v = grad_value_sum.reshape(group_len, head_cols).astype(jnp.bfloat16)
    grad_qkv = jnp.concatenate([grad_q, grad_k, grad_v], axis=1)
    grad_qkv_w = left_dot(h_one_full, grad_qkv)
    grad_wq = grad_qkv_w[:, :head_cols] * score_scale
    grad_wk = grad_qkv_w[:, head_cols : 2 * head_cols]
    grad_wv = grad_qkv_w[:, 2 * head_cols :]
    grad_bias_query = jnp.sum(grad_q.astype(jnp.float32), axis=0) * score_scale
    grad_bias_value = jnp.sum(grad_v.astype(jnp.float32), axis=0)
    grad_h_one = lax.psum_scatter(
        (
            back_dot(grad_qkv[:, :head_cols], full_query) * score_scale
            + back_dot(grad_qkv[:, head_cols:], w_kv)
        ).astype(jnp.bfloat16),
        "tensor",
        scatter_dimension=0,
        tiled=True,
    ).astype(jnp.float32)
    grad_in_norm, grad_gain_one, grad_shift_one = norm_one_back(grad_h_one)
    input_grad = (grad_resid + grad_in_norm).astype(jnp.bfloat16)
    sent_query, sent_key, sent_value, sent_out, sent_up, sent_down = (
        lax.psum_scatter(
            grad_wq.astype(jnp.bfloat16), "dp", scatter_dimension=0, tiled=True
        ).astype(jnp.float32),
        lax.psum_scatter(
            grad_wk.astype(jnp.bfloat16), "dp", scatter_dimension=0, tiled=True
        ).astype(jnp.float32),
        lax.psum_scatter(
            grad_wv.astype(jnp.bfloat16), "dp", scatter_dimension=0, tiled=True
        ).astype(jnp.float32),
        lax.psum_scatter(
            grad_out_w.astype(jnp.bfloat16), "dp", scatter_dimension=1, tiled=True
        ).astype(jnp.float32),
        lax.psum_scatter(
            grad_up.astype(jnp.bfloat16), "dp", scatter_dimension=0, tiled=True
        ).astype(jnp.float32),
        lax.psum_scatter(
            grad_down.astype(jnp.bfloat16), "dp", scatter_dimension=1, tiled=True
        ).astype(jnp.float32),
    )
    summed_query, summed_value, summed_up = lax.psum(
        (grad_bias_query, grad_bias_value, grad_bias_up), "dp"
    )
    gain_one_sum, shift_one_sum, gain_two_sum, shift_two_sum, bias_out_sum, bias_down_sum = (
        lax.psum(
            (
                grad_gain_one,
                grad_shift_one,
                grad_gain_two,
                grad_shift_two,
                grad_bias_out,
                grad_bias_down,
            ),
            ("dp", "tensor"),
        )
    )
    return (
        output,
        input_grad,
        gain_one_sum,
        shift_one_sum,
        sent_query,
        summed_query,
        sent_key,
        sent_value,
        summed_value,
        sent_out,
        bias_out_sum,
        gain_two_sum,
        shift_two_sum,
        sent_up,
        summed_up,
        sent_down,
        bias_down_sum,
    )


def attend_rows(perm_ref, qkv_ref, seg_col_ref, seg_row_ref, out_ref, log_ref, *, count, rows):
    for at in range(count):
        place = pl.multiple_of(perm_ref[at] * rows, rows)
        query = qkv_ref[pl.ds(place, rows), :HDIM]
        scores = []
        for key_at in range(at + 1):
            key_place = pl.multiple_of(perm_ref[key_at] * rows, rows)
            score = back_dot(query, qkv_ref[pl.ds(key_place, rows), HDIM : 2 * HDIM])
            allowed = block_allowed(seg_col_ref, seg_row_ref, at, key_at, rows)
            scores.append(jnp.where(allowed, score, NEG))
        row_top = functools.reduce(
            jnp.maximum, [jnp.max(score, axis=-1, keepdims=True) for score in scores]
        )
        raised = [jnp.exp(score - row_top) for score in scores]
        row_total = sum(jnp.sum(item, axis=-1, keepdims=True) for item in raised)
        inverse = 1.0 / row_total
        mixed = jnp.zeros((rows, HDIM), jnp.float32)
        for key_at in range(at + 1):
            key_place = pl.multiple_of(perm_ref[key_at] * rows, rows)
            mixed = mixed + row_dot(
                (raised[key_at] * inverse).astype(jnp.bfloat16),
                qkv_ref[pl.ds(key_place, rows), 2 * HDIM :],
            )
        out_ref[pl.ds(place, rows), :] = mixed.astype(jnp.bfloat16)
        log_ref[0, at * rows : (at + 1) * rows, :] = row_top + jnp.log(row_total)


def block_allowed(seg_col_ref, seg_row_ref, at, key_at, rows):
    seg_query = seg_col_ref[at * rows : (at + 1) * rows, :]
    seg_key = seg_row_ref[:, key_at * rows : (key_at + 1) * rows]
    shared = (seg_key == seg_query) | (seg_key == 0)
    if at > key_at:
        return shared
    query_pos = lax.broadcasted_iota(jnp.int32, (rows, rows), 0)
    key_pos = lax.broadcasted_iota(jnp.int32, (rows, rows), 1)
    return shared & (key_pos <= query_pos)


def attend_rows_back(
    perm_ref, qkv_ref, grad_ref, log_ref, seg_col_ref, seg_row_ref, out_ref, sum_ref,
    weight_ref, slope_ref, key_sum_ref, value_sum_ref, *, count, rows, score_scale,
):
    query_total = jnp.zeros((1, HDIM), jnp.float32)
    for at in range(count):
        place = pl.multiple_of(perm_ref[at] * rows, rows)
        query = qkv_ref[pl.ds(place, rows), :HDIM]
        grad_out = grad_ref[pl.ds(place, rows), :]
        log_total = log_ref[0, at * rows : (at + 1) * rows, :]
        inner = jnp.zeros((rows, 1), jnp.float32)
        for key_at in range(at + 1):
            key_place = pl.multiple_of(perm_ref[key_at] * rows, rows)
            span = slice(key_at * rows, (key_at + 1) * rows)
            score = back_dot(query, qkv_ref[pl.ds(key_place, rows), HDIM : 2 * HDIM])
            allowed = block_allowed(seg_col_ref, seg_row_ref, at, key_at, rows)
            weight = jnp.exp(jnp.where(allowed, score - log_total, NEG))
            slope = back_dot(grad_out, qkv_ref[pl.ds(key_place, rows), 2 * HDIM :])
            inner = inner + jnp.sum(weight * slope, axis=-1, keepdims=True)
            weight_ref[:, span] = weight
            slope_ref[:, span] = slope
        grad_query = jnp.zeros((rows, HDIM), jnp.float32)
        for key_at in range(at + 1):
            key_place = pl.multiple_of(perm_ref[key_at] * rows, rows)
            span = slice(key_at * rows, (key_at + 1) * rows)
            weight = weight_ref[:, span]
            grad_score = (weight * (slope_ref[:, span] - inner)).astype(jnp.bfloat16)
            grad_query = grad_query + row_dot(
                grad_score, qkv_ref[pl.ds(key_place, rows), HDIM : 2 * HDIM]
            )
            key_part = left_dot(grad_score, query)
            value_part = left_dot(weight.astype(jnp.bfloat16), grad_out)
            if at > key_at:
                key_part = key_part + key_sum_ref[span, :]
                value_part = value_part + value_sum_ref[span, :]
            key_sum_ref[span, :] = key_part
            value_sum_ref[span, :] = value_part
        grad_low = (grad_query * score_scale).astype(jnp.bfloat16)
        out_ref[pl.ds(place, rows), :HDIM] = grad_low
        query_total = query_total + jnp.sum(grad_low.astype(jnp.float32), axis=0, keepdims=True)
    value_total = jnp.zeros((1, HDIM), jnp.float32)
    for at in range(count):
        place = pl.multiple_of(perm_ref[at] * rows, rows)
        span = slice(at * rows, (at + 1) * rows)
        out_ref[pl.ds(place, rows), HDIM : 2 * HDIM] = key_sum_ref[span, :].astype(jnp.bfloat16)
        value_low = value_sum_ref[span, :].astype(jnp.bfloat16)
        out_ref[pl.ds(place, rows), 2 * HDIM :] = value_low
        value_total = value_total + jnp.sum(value_low.astype(jnp.float32), axis=0, keepdims=True)
    sum_ref[0, :, :HDIM] = jnp.broadcast_to(query_total, (8, HDIM))
    sum_ref[0, :, HDIM:] = jnp.broadcast_to(value_total, (8, HDIM))


def attention(perm, qkv, segments):
    length, heads, count = qkv.shape[0], qkv.shape[1] // (3 * HDIM), perm.shape[0]
    pairs = length * length // 2 * HDIM * heads
    return pl.pallas_call(
        functools.partial(attend_rows, count=count, rows=length // count),
        out_shape=(
            jax.ShapeDtypeStruct((length, heads * HDIM), jnp.bfloat16),
            jax.ShapeDtypeStruct((heads, length, 1), jnp.float32),
        ),
        grid_spec=pltpu.PrefetchScalarGridSpec(
            num_scalar_prefetch=1,
            grid=(heads,),
            in_specs=[
                pl.BlockSpec((length, 3 * HDIM), lambda head, perm: (0, head)),
                pl.BlockSpec((length, 1), lambda head, perm: (0, 0)),
                pl.BlockSpec((1, length), lambda head, perm: (0, 0)),
            ],
            out_specs=[
                pl.BlockSpec((length, HDIM), lambda head, perm: (0, head)),
                pl.BlockSpec((1, length, 1), lambda head, perm: (head, 0, 0)),
            ],
        ),
        cost_estimate=pl.CostEstimate(
            flops=4 * pairs, bytes_accessed=8 * length * heads * HDIM, transcendentals=pairs // HDIM
        ),
        name="attention",
    )(perm, qkv, segments.reshape(length, 1), segments.reshape(1, length))


def attention_back(perm, qkv, grad_att, log_total, segments, score_scale):
    length, heads, count = qkv.shape[0], qkv.shape[1] // (3 * HDIM), perm.shape[0]
    rows = length // count
    pairs = length * length // 2 * HDIM * heads
    return pl.pallas_call(
        functools.partial(attend_rows_back, count=count, rows=rows, score_scale=score_scale),
        out_shape=(
            jax.ShapeDtypeStruct(qkv.shape, jnp.bfloat16),
            jax.ShapeDtypeStruct((heads, 8, 2 * HDIM), jnp.float32),
        ),
        grid_spec=pltpu.PrefetchScalarGridSpec(
            num_scalar_prefetch=1,
            grid=(heads,),
            in_specs=[
                pl.BlockSpec((length, 3 * HDIM), lambda head, perm: (0, head)),
                pl.BlockSpec((length, HDIM), lambda head, perm: (0, head)),
                pl.BlockSpec((1, length, 1), lambda head, perm: (head, 0, 0)),
                pl.BlockSpec((length, 1), lambda head, perm: (0, 0)),
                pl.BlockSpec((1, length), lambda head, perm: (0, 0)),
            ],
            out_specs=[
                pl.BlockSpec((length, 3 * HDIM), lambda head, perm: (0, head)),
                pl.BlockSpec((1, 8, 2 * HDIM), lambda head, perm: (head, 0, 0)),
            ],
            scratch_shapes=[
                pltpu.VMEM((rows, length), jnp.float32),
                pltpu.VMEM((rows, length), jnp.float32),
                pltpu.VMEM((length, HDIM), jnp.float32),
                pltpu.VMEM((length, HDIM), jnp.float32),
            ],
        ),
        cost_estimate=pl.CostEstimate(
            flops=10 * pairs, bytes_accessed=16 * length * heads * HDIM, transcendentals=pairs // HDIM
        ),
        name="attention_back",
    )(perm, qkv, grad_att, log_total, segments.reshape(length, 1), segments.reshape(1, length))


def power_of_two(count):
    return count > 0 and count & (count - 1) == 0


def mirrored(value, count):
    bits = count.bit_length() - 1
    out = 0 * value
    for bit in range(bits):
        out = out + ((value >> bit) & 1) * (1 << (bits - 1 - bit))
    return out


def after(values, *marks):
    return lax.optimization_barrier((values, marks))[0]


class Links:
    def __init__(self, mesh):
        self.cols = mesh.shape["tensor"]
        self.ranks = self.cols
        self.halves = mesh.shape["dp"] // self.ranks
        dp_index = lax.axis_index("dp")
        self.half = dp_index // self.ranks
        self.rank = dp_index % self.ranks
        self.col = lax.axis_index("tensor")
        self.quarter = mirrored(self.rank, self.ranks)

    def moved(self, values, target):
        pairs = []
        for half in range(self.halves):
            for rank in range(self.ranks):
                for col in range(self.cols):
                    to_half, to_rank, to_col = target(half, rank, col)
                    pairs.append(
                        (
                            (half * self.ranks + rank) * self.cols + col,
                            (to_half * self.ranks + to_rank) * self.cols + to_col,
                        )
                    )
        return lax.ppermute(values, ("dp", "tensor"), pairs)

    def swap(self, values):
        return self.moved(
            values, lambda half, rank, col: (half, mirrored(col, self.cols), mirrored(rank, self.ranks))
        )

    def rank_pair(self, values, bit):
        return self.moved(values, lambda half, rank, col: (half, rank ^ bit, col))

    def half_pair(self, values, bit):
        return self.moved(values, lambda half, rank, col: (half ^ bit, rank, col))

    def col_pair(self, values, bit):
        return self.moved(values, lambda half, rank, col: (half, rank, col ^ bit))

    def gather_cols(self, values):
        rows = []
        for at in range(self.cols):
            got = values if at == 0 else self.col_pair(values, at)
            place = (jnp.arange(self.cols) == (self.col ^ at)).astype(values.dtype)
            rows.append(place[:, None] * got[None, :])
        return sum(rows)

    def total(self, values):
        for pair, count in (
            (self.rank_pair, self.ranks),
            (self.half_pair, self.halves),
            (self.col_pair, self.cols),
        ):
            bit = 1
            while bit < count:
                values = values + pair(values, bit)
                bit *= 2
        return values

    def rank_bits(self):
        return [1 << place for place in range(self.ranks.bit_length() - 1)]

    def gather_rows(self, piece):
        pieces = {0: piece}
        for bit in reversed(self.rank_bits()):
            for at in list(pieces):
                pieces[at | bit] = self.rank_pair(pieces[at], bit)
        return [pieces[at] for at in range(self.ranks)]

    def scatter_rows(self, pieces):
        sums = dict(enumerate(pieces))
        for bit in self.rank_bits():
            for at in [item for item in sums if item & bit]:
                arrived = self.rank_pair(sums.pop(at).astype(jnp.bfloat16), bit)
                sums[at ^ bit] = sums[at ^ bit] + arrived.astype(jnp.float32)
        return sums[0]

    def half_order(self, values, axis):
        if self.halves == 1:
            return values
        width = values.shape[axis] // self.halves
        return jnp.concatenate(
            [
                lax.dynamic_slice_in_dim(values, (self.half ^ at) * width, width, axis)
                for at in range(self.halves)
            ],
            axis=axis,
        )

    def places(self):
        return jnp.stack(
            [mirrored(at ^ self.quarter, self.ranks) for at in range(self.ranks)]
        ).astype(jnp.int32)

    def row_order(self, pieces):
        stacked = jnp.concatenate(pieces, axis=0)
        rows = pieces[0].shape[0]
        return jnp.concatenate(
            [
                lax.dynamic_slice_in_dim(
                    stacked, mirrored(at ^ self.quarter, self.ranks) * rows, rows, 0
                )
                for at in range(self.ranks)
            ],
            axis=0,
        )

    def piece_order(self, values):
        rows = values.shape[0] // self.ranks
        return [
            lax.dynamic_slice_in_dim(
                values, (self.quarter ^ mirrored(at, self.ranks)) * rows, rows, 0
            )
            for at in range(self.ranks)
        ]

    def rank_groups(self):
        return [
            [half * self.ranks + rank for rank in range(self.ranks)] for half in range(self.halves)
        ]

    def spread_ranks(self, shard, hidden_axis):
        return lax.all_to_all(
            shard, "dp", hidden_axis, 1 - hidden_axis, axis_index_groups=self.rank_groups(), tiled=True
        )

    def spread_cols(self, part, hidden_axis):
        return lax.all_gather(part, "tensor", axis=hidden_axis, tiled=True)

    def spread_halves(self, part, hidden_axis):
        parts = {0: part}
        bit = self.halves // 2
        while bit:
            for at in list(parts):
                parts[at | bit] = self.half_pair(parts[at], bit)
            bit //= 2
        return jnp.concatenate([parts[at] for at in range(self.halves)], axis=1 - hidden_axis)

    def collect(self, grad, hidden_axis, *marks):
        other = 1 - hidden_axis
        width = grad.shape[other] // self.halves
        sums = {
            at: lax.slice_in_dim(grad, at * width, (at + 1) * width, axis=other)
            for at in range(self.halves)
        }
        bit = 1
        while bit < self.halves:
            for at in [item for item in sums if item & bit]:
                arrived = self.half_pair(sums.pop(at).astype(jnp.bfloat16), bit)
                if marks:
                    arrived = after(arrived, *marks)
                sums[at ^ bit] = sums[at ^ bit] + arrived.astype(jnp.float32)
            bit *= 2
        part = lax.psum_scatter(
            sums[0].astype(jnp.bfloat16), "tensor", scatter_dimension=hidden_axis, tiled=True
        )
        return lax.all_to_all(
            part, "dp", other, hidden_axis, axis_index_groups=self.rank_groups(), tiled=True
        ).astype(jnp.float32)

    def rank_part(self, values):
        width = values.shape[0] // self.ranks
        return lax.dynamic_slice_in_dim(values, self.rank * width, width, 0)

    def rank_slots(self, values):
        mine = (jnp.arange(self.ranks) == self.rank).astype(values.dtype)
        blocks = values.reshape(self.cols, 1, -1)
        return (blocks * mine[None, :, None]).reshape(-1)


def swapped_on_device(
    mesh,
    tokens,
    segments,
    cotangent,
    ln1_gain,
    ln1_shift,
    w_query,
    b_query,
    w_key,
    w_value,
    b_value,
    w_out,
    b_out,
    ln2_gain,
    ln2_shift,
    w_up,
    b_up,
    w_down,
    b_down,
):
    links = Links(mesh)
    ranks, cols = links.ranks, links.cols
    score_scale = 1.0 / math.sqrt(HDIM)
    group_len = segments.shape[0]
    head_cols = w_query.shape[1]
    heads_here = head_cols // HDIM
    sub_cols = head_cols // ranks
    block_count = group_len // QBLK
    f32 = jnp.float32
    low = jnp.bfloat16

    tokens = links.half_order(links.swap(tokens), 1)
    segments = links.swap(segments)

    w_qkv_shard = jnp.concatenate(
        [item.reshape(-1, ranks, sub_cols) for item in (w_query, w_key, w_value)], axis=2
    ).reshape(w_query.shape[0], -1)
    biases = jnp.concatenate([links.rank_part(item) for item in (b_query, b_value, b_up)])
    biases = links.gather_cols(biases.astype(f32))
    bias_query = biases[:, :sub_cols].reshape(-1)
    bias_value = biases[:, sub_cols : 2 * sub_cols].reshape(-1)
    bias_up = biases[:, 2 * sub_cols :].reshape(-1)
    part_qkv = links.spread_ranks(w_qkv_shard, 1)
    part_out, part_up, part_down = (
        links.spread_ranks(after(shard, part_qkv), axis)
        for shard, axis in ((w_out, 0), (w_up, 1), (w_down, 0))
    )
    part_qkv = links.spread_cols(part_qkv, 1)
    full_qkv = links.spread_halves(part_qkv, 1)
    part_out = links.spread_cols(part_out, 0)
    part_up = links.spread_cols(after(part_up, part_qkv), 1)
    part_down = links.spread_cols(after(part_down, part_out), 0)
    full_out = links.spread_halves(part_out, 0)

    gain_one, shift_one, gain_two, shift_two, out_bias, down_bias = (
        links.half_order(item.astype(f32), 0)
        for item in (ln1_gain, ln1_shift, ln2_gain, ln2_shift, b_out, b_down)
    )

    inputs = tokens.astype(f32)
    normed_one, norm_one_back = jax.vjp(layer_norm, inputs, gain_one, shift_one)
    h_one_pieces = links.gather_rows(normed_one.astype(low))
    blocks = (heads_here, 1, HDIM)
    no_bias = jnp.zeros(blocks, f32)
    qkv_bias = jnp.concatenate(
        [bias_query.reshape(blocks), no_bias, bias_value.reshape(blocks)], axis=1
    ).reshape(-1)
    qkv_scale = jnp.concatenate(
        [jnp.full(blocks, score_scale, f32), jnp.ones((heads_here, 2, HDIM), f32)], axis=1
    ).reshape(-1)
    qkv = jnp.concatenate(
        [((row_dot(piece, full_qkv) + qkv_bias) * qkv_scale).astype(low) for piece in h_one_pieces],
        axis=0,
    )
    places = links.places()
    grad_y_low = links.half_order(links.swap(cotangent), 1)
    grad_y = grad_y_low.astype(f32)
    grad_y_pieces = links.gather_rows(grad_y_low)
    attended, log_total = attention(places, qkv, segments)
    attended = after(attended, *grad_y_pieces)
    full_up = links.spread_halves(after(part_up, attended), 1)
    rows = tokens.shape[0]
    attended_pieces = [attended[at * rows : (at + 1) * rows] for at in range(ranks)]
    resid = (
        inputs
        + links.scatter_rows([row_dot(piece, full_out) for piece in attended_pieces])
        + out_bias
    )
    normed_two, norm_two_back = jax.vjp(layer_norm, resid, gain_two, shift_two)
    h_two = jnp.concatenate(links.gather_rows(normed_two.astype(low)), axis=0)
    full_down = links.spread_halves(after(part_down, resid), 0)
    pre_act = row_dot(h_two, full_up) + bias_up
    activated, gelu_back = jax.vjp(gelu_exact, pre_act)
    act_low = activated.astype(low)
    grad_y_full = jnp.concatenate(grad_y_pieces, axis=0)
    grad_w_down = left_dot(act_low, grad_y_full)
    grad_act = back_dot(grad_y_full, full_down)
    grad_pre = gelu_back(grad_act)[0].astype(low)
    grad_bias_up = jnp.sum(grad_pre.astype(f32), axis=0)
    grad_w_up = left_dot(h_two, grad_pre)
    grad_h_two = links.scatter_rows(
        [back_dot(grad_pre[at * rows : (at + 1) * rows], full_up) for at in range(ranks)]
    )
    grad_resid_norm, grad_gain_two, grad_shift_two = norm_two_back(grad_h_two)
    grad_resid = grad_y + grad_resid_norm
    grad_mix = grad_resid.astype(low)
    grad_bias_out = jnp.sum(grad_mix.astype(f32), axis=0)
    grad_bias_down = jnp.sum(grad_y, axis=0)
    grad_mix_pieces = links.gather_rows(grad_mix)
    grad_mix_full = jnp.concatenate(grad_mix_pieces, axis=0)
    down_pieces = [
        row_dot(act_low[at * rows : (at + 1) * rows], full_down) for at in range(ranks)
    ]
    down_pieces = after(down_pieces, grad_mix_pieces[-1])
    output = (resid + links.scatter_rows(down_pieces) + down_bias).astype(low)
    output = links.swap(links.half_order(output, 1))
    grad_w_out = left_dot(attended, grad_mix_full)
    grad_att = jnp.concatenate(
        [back_dot(piece, full_out).astype(low) for piece in grad_mix_pieces], axis=0
    )
    grad_qkv, bias_sums = attention_back(places, qkv, grad_att, log_total, segments, score_scale)
    sent_down = links.collect(grad_w_down, 0, grad_att)
    sent_up = links.collect(grad_w_up, 1, grad_qkv)
    sent_out = links.collect(grad_w_out, 0, grad_qkv)
    grad_bias_query = bias_sums[:, 0, :HDIM].reshape(-1)
    grad_bias_value = bias_sums[:, 0, HDIM:].reshape(-1)
    grad_w_qkv = left_dot(jnp.concatenate(h_one_pieces, axis=0), grad_qkv)
    sent_qkv = links.collect(grad_w_qkv, 1).reshape(w_query.shape[0], ranks, 3, sub_cols)
    sent_query, sent_key, sent_value = (
        sent_qkv[:, :, at].reshape(w_query.shape) for at in range(3)
    )
    grad_h_one = links.scatter_rows(
        [back_dot(grad_qkv[at * rows : (at + 1) * rows], full_qkv) for at in range(ranks)]
    )
    grad_in_norm, grad_gain_one, grad_shift_one = norm_one_back(grad_h_one)
    input_grad = (grad_resid + grad_in_norm).astype(low)
    input_grad = links.swap(links.half_order(input_grad, 1))

    def my_block(values):
        width = values.shape[0] // cols
        return lax.dynamic_slice_in_dim(values, links.col * width, width, 0)

    def summed(*vectors):
        packed = links.total(jnp.concatenate(vectors).reshape(-1, 128)).reshape(-1)
        ends = [sum(item.size for item in vectors[: at + 1]) for at in range(len(vectors))]
        return [packed[end - item.size : end] for item, end in zip(vectors, ends)]

    early = summed(
        links.rank_slots(grad_bias_up),
        links.half_order(grad_gain_two, 0),
        links.half_order(grad_shift_two, 0),
        links.half_order(grad_bias_out, 0),
        links.half_order(grad_bias_down, 0),
    )
    late = summed(
        links.rank_slots(grad_bias_query),
        links.rank_slots(grad_bias_value),
        links.half_order(grad_gain_one, 0),
        links.half_order(grad_shift_one, 0),
    )
    return (
        output,
        input_grad,
        late[2],
        late[3],
        sent_query,
        my_block(late[0]),
        sent_key,
        sent_value,
        my_block(late[1]),
        sent_out,
        early[3],
        early[1],
        early[2],
        sent_up,
        my_block(early[0]),
        sent_down,
        early[4],
    )


def can_swap(mesh, head_cols):
    ranks = mesh.shape["tensor"]
    dp_size = mesh.shape["dp"]
    if dp_size % ranks or not power_of_two(ranks) or not power_of_two(dp_size // ranks):
        return False
    return head_cols % (ranks * HDIM) == 0


def either_on_device(mesh):
    def run(*arrays):
        w_query = arrays[5]
        if can_swap(mesh, w_query.shape[1]):
            return swapped_on_device(mesh, *arrays)
        return on_device(*arrays)

    return run


def solution(mesh):
    return jax.shard_map(
        either_on_device(mesh),
        mesh=mesh,
        in_specs=(
            P(("dp", "tensor"), None),
            P("dp"),
            P(("dp", "tensor"), None),
            P(),
            P(),
            P("dp", "tensor"),
            P("tensor"),
            P("dp", "tensor"),
            P("dp", "tensor"),
            P("tensor"),
            P("tensor", "dp"),
            P(),
            P(),
            P(),
            P("dp", "tensor"),
            P("tensor"),
            P("tensor", "dp"),
            P(),
        ),
        out_specs=(
            P(("dp", "tensor"), None),
            P(("dp", "tensor"), None),
            P(),
            P(),
            P("dp", "tensor"),
            P("tensor"),
            P("dp", "tensor"),
            P("dp", "tensor"),
            P("tensor"),
            P("tensor", "dp"),
            P(),
            P(),
            P(),
            P("dp", "tensor"),
            P("tensor"),
            P("tensor", "dp"),
            P(),
        ),
        check_vma=False,
    )
```

```python
import functools
import math

import jax
import jax.numpy as jnp
from jax import lax
from jax.experimental import pallas as pl
from jax.experimental.pallas import tpu as pltpu
from jax.sharding import PartitionSpec as P


HDIM = 128
QBLK = 768


EPS = 1e-05
NEG = -1e30


def layer_norm(values, norm_gain, norm_shift):
    row_mean = jnp.mean(values, axis=-1, keepdims=True)
    centred = values - row_mean
    row_var = jnp.mean(centred * centred, axis=-1, keepdims=True)
    return centred * lax.rsqrt(row_var + EPS) * norm_gain + norm_shift


def gelu_exact(values):
    return jax.nn.gelu(values, approximate=False)


def row_dot(left_side, right_side):
    return jnp.dot(left_side, right_side, preferred_element_type=jnp.float32)


def left_dot(left_side, right_side):
    return lax.dot_general(
        left_side, right_side, (((0,), (0,)), ((), ())), preferred_element_type=jnp.float32
    )


def back_dot(left_side, right_side):
    return lax.dot_general(
        left_side, right_side, (((1,), (1,)), ((), ())), preferred_element_type=jnp.float32
    )


def visible(segments, first_row, row_count, key_end):
    query_pos = first_row + jnp.arange(row_count)
    key_pos = jnp.arange(key_end)
    seg_query = segments[first_row : first_row + row_count]
    seg_key = segments[:key_end]
    causal = key_pos[None, :] <= query_pos[:, None]
    shared = (seg_key[None, :] == seg_query[:, None]) | (seg_key[None, :] == 0)
    return causal & shared


def attend_block(queries, key_rows, value_rows, allowed):
    scores = jnp.einsum("qhd,khd->hqk", queries, key_rows, preferred_element_type=jnp.float32)
    scores = jnp.where(allowed[None], scores, NEG)
    row_top = jnp.max(scores, axis=-1, keepdims=True)
    raised = jnp.exp(scores - row_top)
    row_total = jnp.sum(raised, axis=-1, keepdims=True)
    weights = raised / row_total
    mixed = jnp.einsum(
        "hqk,khd->qhd", weights.astype(jnp.bfloat16), value_rows, preferred_element_type=jnp.float32
    )
    return (mixed.astype(jnp.bfloat16), row_top + jnp.log(row_total))


def attend_back(queries, key_rows, value_rows, grad_out, log_total, allowed):
    scores = jnp.einsum("qhd,khd->hqk", queries, key_rows, preferred_element_type=jnp.float32)
    weights = jnp.where(allowed[None], jnp.exp(scores - log_total), 0.0)
    grad_weights = jnp.einsum(
        "qhd,khd->hqk", grad_out, value_rows, preferred_element_type=jnp.float32
    )
    inner = jnp.sum(weights * grad_weights, axis=-1, keepdims=True)
    grad_scores = (weights * (grad_weights - inner)).astype(jnp.bfloat16)
    grad_query = jnp.einsum(
        "hqk,khd->qhd", grad_scores, key_rows, preferred_element_type=jnp.float32
    )
    grad_key = jnp.einsum("hqk,qhd->khd", grad_scores, queries, preferred_element_type=jnp.float32)
    grad_value = jnp.einsum(
        "hqk,qhd->khd", weights.astype(jnp.bfloat16), grad_out, preferred_element_type=jnp.float32
    )
    return (grad_query, grad_key, grad_value)


def on_device(
    tokens,
    segments,
    cotangent,
    ln1_gain,
    ln1_shift,
    w_query,
    b_query,
    w_key,
    w_value,
    b_value,
    w_out,
    b_out,
    ln2_gain,
    ln2_shift,
    w_up,
    b_up,
    w_down,
    b_down,
):
    score_scale = 1.0 / math.sqrt(HDIM)
    full_query, full_key, full_value, full_out, full_up, full_down = (
        lax.all_gather(w_query, "dp", axis=0, tiled=True),
        lax.all_gather(w_key, "dp", axis=0, tiled=True),
        lax.all_gather(w_value, "dp", axis=0, tiled=True),
        lax.all_gather(w_out, "dp", axis=1, tiled=True),
        lax.all_gather(w_up, "dp", axis=0, tiled=True),
        lax.all_gather(w_down, "dp", axis=1, tiled=True),
    )
    group_len = segments.shape[0]
    head_cols = full_query.shape[1]
    heads_here = head_cols // HDIM
    block_count = group_len // QBLK
    inputs = tokens.astype(jnp.float32)
    normed_one, norm_one_back = jax.vjp(
        layer_norm, inputs, ln1_gain.astype(jnp.float32), ln1_shift.astype(jnp.float32)
    )
    h_one = normed_one.astype(jnp.bfloat16)
    h_one_full = lax.all_gather(h_one, "tensor", axis=0, tiled=True)
    w_qkv = jnp.concatenate([full_query, full_key, full_value], axis=1)
    w_kv = w_qkv[:, head_cols:]
    projected = row_dot(h_one_full, w_qkv)
    queries = ((projected[:, :head_cols] + b_query.astype(jnp.float32)) * score_scale).astype(
        jnp.bfloat16
    )
    key_rows = projected[:, head_cols : 2 * head_cols].astype(jnp.bfloat16)
    value_rows = (projected[:, 2 * head_cols :] + b_value.astype(jnp.float32)).astype(jnp.bfloat16)
    query3 = queries.reshape(group_len, heads_here, HDIM)
    key3 = key_rows.reshape(group_len, heads_here, HDIM)
    value3 = value_rows.reshape(group_len, heads_here, HDIM)
    pieces = []
    totals = []
    for block in range(block_count):
        first_row = block * QBLK
        key_end = first_row + QBLK
        allowed = visible(segments, first_row, QBLK, key_end)
        mixed_block, log_total = attend_block(
            query3[first_row:key_end], key3[:key_end], value3[:key_end], allowed
        )
        pieces.append(mixed_block)
        totals.append(log_total)
    attended = jnp.concatenate(pieces, axis=0).reshape(group_len, head_cols)
    resid = (
        inputs
        + lax.psum_scatter(row_dot(attended, full_out), "tensor", scatter_dimension=0, tiled=True)
        + b_out.astype(jnp.float32)
    )
    normed_two, norm_two_back = jax.vjp(
        layer_norm, resid, ln2_gain.astype(jnp.float32), ln2_shift.astype(jnp.float32)
    )
    h_two = normed_two.astype(jnp.bfloat16)
    h_two_full = lax.all_gather(h_two, "tensor", axis=0, tiled=True)
    pre_act = row_dot(h_two_full, full_up) + b_up.astype(jnp.float32)
    activated, gelu_back = jax.vjp(gelu_exact, pre_act)
    act_low = activated.astype(jnp.bfloat16)
    output = (
        resid
        + lax.psum_scatter(
            row_dot(act_low, full_down).astype(jnp.bfloat16),
            "tensor",
            scatter_dimension=0,
            tiled=True,
        ).astype(jnp.float32)
        + b_down.astype(jnp.float32)
    ).astype(jnp.bfloat16)
    grad_y = cotangent.astype(jnp.float32)
    grad_y_full = lax.all_gather(cotangent, "tensor", axis=0, tiled=True)
    grad_down = left_dot(act_low, grad_y_full)
    grad_act = back_dot(grad_y_full, full_down)
    grad_pre = gelu_back(grad_act)[0].astype(jnp.bfloat16)
    grad_bias_up = jnp.sum(grad_pre.astype(jnp.float32), axis=0)
    grad_up = left_dot(h_two_full, grad_pre)
    grad_h_two = lax.psum_scatter(
        back_dot(grad_pre, full_up), "tensor", scatter_dimension=0, tiled=True
    )
    grad_resid_norm, grad_gain_two, grad_shift_two = norm_two_back(grad_h_two)
    grad_resid = grad_y + grad_resid_norm
    grad_mix = grad_resid.astype(jnp.bfloat16)
    grad_bias_out = jnp.sum(grad_mix.astype(jnp.float32), axis=0)
    grad_bias_down = jnp.sum(grad_y, axis=0)
    grad_mix_full = lax.all_gather(grad_mix, "tensor", axis=0, tiled=True)
    grad_out_w = left_dot(attended, grad_mix_full)
    grad_att = (
        back_dot(grad_mix_full, full_out).astype(jnp.bfloat16).reshape(group_len, heads_here, HDIM)
    )
    grad_key_sum = jnp.zeros((group_len, heads_here, HDIM), jnp.float32)
    grad_value_sum = jnp.zeros((group_len, heads_here, HDIM), jnp.float32)
    query_grads = []
    for block in range(block_count):
        first_row = block * QBLK
        key_end = first_row + QBLK
        allowed = visible(segments, first_row, QBLK, key_end)
        grad_q_block, grad_k_part, grad_v_part = attend_back(
            query3[first_row:key_end],
            key3[:key_end],
            value3[:key_end],
            grad_att[first_row:key_end],
            totals[block],
            allowed,
        )
        query_grads.append(grad_q_block.astype(jnp.bfloat16))
        grad_key_sum = grad_key_sum.at[:key_end].add(grad_k_part)
        grad_value_sum = grad_value_sum.at[:key_end].add(grad_v_part)
    grad_q = jnp.concatenate(query_grads, axis=0).reshape(group_len, head_cols)
    grad_k = grad_key_sum.reshape(group_len, head_cols).astype(jnp.bfloat16)
    grad_v = grad_value_sum.reshape(group_len, head_cols).astype(jnp.bfloat16)
    grad_qkv = jnp.concatenate([grad_q, grad_k, grad_v], axis=1)
    grad_qkv_w = left_dot(h_one_full, grad_qkv)
    grad_wq = grad_qkv_w[:, :head_cols] * score_scale
    grad_wk = grad_qkv_w[:, head_cols : 2 * head_cols]
    grad_wv = grad_qkv_w[:, 2 * head_cols :]
    grad_bias_query = jnp.sum(grad_q.astype(jnp.float32), axis=0) * score_scale
    grad_bias_value = jnp.sum(grad_v.astype(jnp.float32), axis=0)
    grad_h_one = lax.psum_scatter(
        (
            back_dot(grad_qkv[:, :head_cols], full_query) * score_scale
            + back_dot(grad_qkv[:, head_cols:], w_kv)
        ).astype(jnp.bfloat16),
        "tensor",
        scatter_dimension=0,
        tiled=True,
    ).astype(jnp.float32)
    grad_in_norm, grad_gain_one, grad_shift_one = norm_one_back(grad_h_one)
    input_grad = (grad_resid + grad_in_norm).astype(jnp.bfloat16)
    sent_query, sent_key, sent_value, sent_out, sent_up, sent_down = (
        lax.psum_scatter(
            grad_wq.astype(jnp.bfloat16), "dp", scatter_dimension=0, tiled=True
        ).astype(jnp.float32),
        lax.psum_scatter(
            grad_wk.astype(jnp.bfloat16), "dp", scatter_dimension=0, tiled=True
        ).astype(jnp.float32),
        lax.psum_scatter(
            grad_wv.astype(jnp.bfloat16), "dp", scatter_dimension=0, tiled=True
        ).astype(jnp.float32),
        lax.psum_scatter(
            grad_out_w.astype(jnp.bfloat16), "dp", scatter_dimension=1, tiled=True
        ).astype(jnp.float32),
        lax.psum_scatter(
            grad_up.astype(jnp.bfloat16), "dp", scatter_dimension=0, tiled=True
        ).astype(jnp.float32),
        lax.psum_scatter(
            grad_down.astype(jnp.bfloat16), "dp", scatter_dimension=1, tiled=True
        ).astype(jnp.float32),
    )
    summed_query, summed_value, summed_up = lax.psum(
        (grad_bias_query, grad_bias_value, grad_bias_up), "dp"
    )
    gain_one_sum, shift_one_sum, gain_two_sum, shift_two_sum, bias_out_sum, bias_down_sum = (
        lax.psum(
            (
                grad_gain_one,
                grad_shift_one,
                grad_gain_two,
                grad_shift_two,
                grad_bias_out,
                grad_bias_down,
            ),
            ("dp", "tensor"),
        )
    )
    return (
        output,
        input_grad,
        gain_one_sum,
        shift_one_sum,
        sent_query,
        summed_query,
        sent_key,
        sent_value,
        summed_value,
        sent_out,
        bias_out_sum,
        gain_two_sum,
        shift_two_sum,
        sent_up,
        summed_up,
        sent_down,
        bias_down_sum,
    )


def attend_rows(perm_ref, qkv_ref, seg_col_ref, seg_row_ref, out_ref, log_ref, *, count, rows):
    for at in range(count):
        place = pl.multiple_of(perm_ref[at] * rows, rows)
        query = qkv_ref[pl.ds(place, rows), :HDIM]
        scores = []
        for key_at in range(at + 1):
            key_place = pl.multiple_of(perm_ref[key_at] * rows, rows)
            score = back_dot(query, qkv_ref[pl.ds(key_place, rows), HDIM : 2 * HDIM])
            allowed = block_allowed(seg_col_ref, seg_row_ref, at, key_at, rows)
            scores.append(jnp.where(allowed, score, NEG))
        row_top = functools.reduce(
            jnp.maximum, [jnp.max(score, axis=-1, keepdims=True) for score in scores]
        )
        raised = [jnp.exp(score - row_top) for score in scores]
        row_total = sum(jnp.sum(item, axis=-1, keepdims=True) for item in raised)
        inverse = 1.0 / row_total
        mixed = jnp.zeros((rows, HDIM), jnp.float32)
        for key_at in range(at + 1):
            key_place = pl.multiple_of(perm_ref[key_at] * rows, rows)
            mixed = mixed + row_dot(
                (raised[key_at] * inverse).astype(jnp.bfloat16),
                qkv_ref[pl.ds(key_place, rows), 2 * HDIM :],
            )
        out_ref[pl.ds(place, rows), :] = mixed.astype(jnp.bfloat16)
        log_ref[0, at * rows : (at + 1) * rows, :] = row_top + jnp.log(row_total)


def block_allowed(seg_col_ref, seg_row_ref, at, key_at, rows):
    seg_query = seg_col_ref[at * rows : (at + 1) * rows, :]
    seg_key = seg_row_ref[:, key_at * rows : (key_at + 1) * rows]
    shared = (seg_key == seg_query) | (seg_key == 0)
    if at > key_at:
        return shared
    query_pos = lax.broadcasted_iota(jnp.int32, (rows, rows), 0)
    key_pos = lax.broadcasted_iota(jnp.int32, (rows, rows), 1)
    return shared & (key_pos <= query_pos)


def attend_rows_back(
    perm_ref, qkv_ref, grad_ref, log_ref, seg_col_ref, seg_row_ref, out_ref, sum_ref,
    weight_ref, slope_ref, key_sum_ref, value_sum_ref, *, count, rows, score_scale,
):
    query_total = jnp.zeros((1, HDIM), jnp.float32)
    for at in range(count):
        place = pl.multiple_of(perm_ref[at] * rows, rows)
        query = qkv_ref[pl.ds(place, rows), :HDIM]
        grad_out = grad_ref[pl.ds(place, rows), :]
        log_total = log_ref[0, at * rows : (at + 1) * rows, :]
        inner = jnp.zeros((rows, 1), jnp.float32)
        for key_at in range(at + 1):
            key_place = pl.multiple_of(perm_ref[key_at] * rows, rows)
            span = slice(key_at * rows, (key_at + 1) * rows)
            score = back_dot(query, qkv_ref[pl.ds(key_place, rows), HDIM : 2 * HDIM])
            allowed = block_allowed(seg_col_ref, seg_row_ref, at, key_at, rows)
            weight = jnp.exp(jnp.where(allowed, score - log_total, NEG))
            slope = back_dot(grad_out, qkv_ref[pl.ds(key_place, rows), 2 * HDIM :])
            inner = inner + jnp.sum(weight * slope, axis=-1, keepdims=True)
            weight_ref[:, span] = weight
            slope_ref[:, span] = slope
        grad_query = jnp.zeros((rows, HDIM), jnp.float32)
        for key_at in range(at + 1):
            key_place = pl.multiple_of(perm_ref[key_at] * rows, rows)
            span = slice(key_at * rows, (key_at + 1) * rows)
            weight = weight_ref[:, span]
            grad_score = (weight * (slope_ref[:, span] - inner)).astype(jnp.bfloat16)
            grad_query = grad_query + row_dot(
                grad_score, qkv_ref[pl.ds(key_place, rows), HDIM : 2 * HDIM]
            )
            key_part = left_dot(grad_score, query)
            value_part = left_dot(weight.astype(jnp.bfloat16), grad_out)
            if at > key_at:
                key_part = key_part + key_sum_ref[span, :]
                value_part = value_part + value_sum_ref[span, :]
            key_sum_ref[span, :] = key_part
            value_sum_ref[span, :] = value_part
        grad_low = (grad_query * score_scale).astype(jnp.bfloat16)
        out_ref[pl.ds(place, rows), :HDIM] = grad_low
        query_total = query_total + jnp.sum(grad_low.astype(jnp.float32), axis=0, keepdims=True)
    value_total = jnp.zeros((1, HDIM), jnp.float32)
    for at in range(count):
        place = pl.multiple_of(perm_ref[at] * rows, rows)
        span = slice(at * rows, (at + 1) * rows)
        out_ref[pl.ds(place, rows), HDIM : 2 * HDIM] = key_sum_ref[span, :].astype(jnp.bfloat16)
        value_low = value_sum_ref[span, :].astype(jnp.bfloat16)
        out_ref[pl.ds(place, rows), 2 * HDIM :] = value_low
        value_total = value_total + jnp.sum(value_low.astype(jnp.float32), axis=0, keepdims=True)
    sum_ref[0, :, :HDIM] = jnp.broadcast_to(query_total, (8, HDIM))
    sum_ref[0, :, HDIM:] = jnp.broadcast_to(value_total, (8, HDIM))


def attention(perm, qkv, segments):
    length, heads, count = qkv.shape[0], qkv.shape[1] // (3 * HDIM), perm.shape[0]
    pairs = length * length // 2 * HDIM * heads
    return pl.pallas_call(
        functools.partial(attend_rows, count=count, rows=length // count),
        out_shape=(
            jax.ShapeDtypeStruct((length, heads * HDIM), jnp.bfloat16),
            jax.ShapeDtypeStruct((heads, length, 1), jnp.float32),
        ),
        grid_spec=pltpu.PrefetchScalarGridSpec(
            num_scalar_prefetch=1,
            grid=(heads,),
            in_specs=[
                pl.BlockSpec((length, 3 * HDIM), lambda head, perm: (0, head)),
                pl.BlockSpec((length, 1), lambda head, perm: (0, 0)),
                pl.BlockSpec((1, length), lambda head, perm: (0, 0)),
            ],
            out_specs=[
                pl.BlockSpec((length, HDIM), lambda head, perm: (0, head)),
                pl.BlockSpec((1, length, 1), lambda head, perm: (head, 0, 0)),
            ],
        ),
        cost_estimate=pl.CostEstimate(
            flops=4 * pairs, bytes_accessed=8 * length * heads * HDIM, transcendentals=pairs // HDIM
        ),
        name="attention",
    )(perm, qkv, segments.reshape(length, 1), segments.reshape(1, length))


def attention_back(perm, qkv, grad_att, log_total, segments, score_scale):
    length, heads, count = qkv.shape[0], qkv.shape[1] // (3 * HDIM), perm.shape[0]
    rows = length // count
    pairs = length * length // 2 * HDIM * heads
    return pl.pallas_call(
        functools.partial(attend_rows_back, count=count, rows=rows, score_scale=score_scale),
        out_shape=(
            jax.ShapeDtypeStruct(qkv.shape, jnp.bfloat16),
            jax.ShapeDtypeStruct((heads, 8, 2 * HDIM), jnp.float32),
        ),
        grid_spec=pltpu.PrefetchScalarGridSpec(
            num_scalar_prefetch=1,
            grid=(heads,),
            in_specs=[
                pl.BlockSpec((length, 3 * HDIM), lambda head, perm: (0, head)),
                pl.BlockSpec((length, HDIM), lambda head, perm: (0, head)),
                pl.BlockSpec((1, length, 1), lambda head, perm: (head, 0, 0)),
                pl.BlockSpec((length, 1), lambda head, perm: (0, 0)),
                pl.BlockSpec((1, length), lambda head, perm: (0, 0)),
            ],
            out_specs=[
                pl.BlockSpec((length, 3 * HDIM), lambda head, perm: (0, head)),
                pl.BlockSpec((1, 8, 2 * HDIM), lambda head, perm: (head, 0, 0)),
            ],
            scratch_shapes=[
                pltpu.VMEM((rows, length), jnp.float32),
                pltpu.VMEM((rows, length), jnp.float32),
                pltpu.VMEM((length, HDIM), jnp.float32),
                pltpu.VMEM((length, HDIM), jnp.float32),
            ],
        ),
        cost_estimate=pl.CostEstimate(
            flops=10 * pairs, bytes_accessed=16 * length * heads * HDIM, transcendentals=pairs // HDIM
        ),
        name="attention_back",
    )(perm, qkv, grad_att, log_total, segments.reshape(length, 1), segments.reshape(1, length))


def power_of_two(count):
    return count > 0 and count & (count - 1) == 0


def mirrored(value, count):
    bits = count.bit_length() - 1
    out = 0 * value
    for bit in range(bits):
        out = out + ((value >> bit) & 1) * (1 << (bits - 1 - bit))
    return out


def after(values, *marks):
    return lax.optimization_barrier((values, marks))[0]


class Links:
    def __init__(self, mesh):
        self.cols = mesh.shape["tensor"]
        self.ranks = self.cols
        self.halves = mesh.shape["dp"] // self.ranks
        dp_index = lax.axis_index("dp")
        self.half = dp_index // self.ranks
        self.rank = dp_index % self.ranks
        self.col = lax.axis_index("tensor")
        self.quarter = mirrored(self.rank, self.ranks)

    def moved(self, values, target):
        pairs = []
        for half in range(self.halves):
            for rank in range(self.ranks):
                for col in range(self.cols):
                    to_half, to_rank, to_col = target(half, rank, col)
                    pairs.append(
                        (
                            (half * self.ranks + rank) * self.cols + col,
                            (to_half * self.ranks + to_rank) * self.cols + to_col,
                        )
                    )
        return lax.ppermute(values, ("dp", "tensor"), pairs)

    def swap(self, values):
        return self.moved(
            values, lambda half, rank, col: (half, mirrored(col, self.cols), mirrored(rank, self.ranks))
        )

    def rank_pair(self, values, bit):
        return self.moved(values, lambda half, rank, col: (half, rank ^ bit, col))

    def half_pair(self, values, bit):
        return self.moved(values, lambda half, rank, col: (half ^ bit, rank, col))

    def col_pair(self, values, bit):
        return self.moved(values, lambda half, rank, col: (half, rank, col ^ bit))

    def gather_cols(self, values):
        rows = []
        for at in range(self.cols):
            got = values if at == 0 else self.col_pair(values, at)
            place = (jnp.arange(self.cols) == (self.col ^ at)).astype(values.dtype)
            rows.append(place[:, None] * got[None, :])
        return sum(rows)

    def total(self, values):
        for pair, count in (
            (self.rank_pair, self.ranks),
            (self.half_pair, self.halves),
            (self.col_pair, self.cols),
        ):
            bit = 1
            while bit < count:
                values = values + pair(values, bit)
                bit *= 2
        return values

    def rank_bits(self):
        return [1 << place for place in range(self.ranks.bit_length() - 1)]

    def gather_rows(self, piece):
        pieces = {0: piece}
        for bit in reversed(self.rank_bits()):
            for at in list(pieces):
                pieces[at | bit] = self.rank_pair(pieces[at], bit)
        return [pieces[at] for at in range(self.ranks)]

    def scatter_rows(self, pieces):
        sums = dict(enumerate(pieces))
        for bit in self.rank_bits():
            for at in [item for item in sums if item & bit]:
                arrived = self.rank_pair(sums.pop(at).astype(jnp.bfloat16), bit)
                sums[at ^ bit] = sums[at ^ bit] + arrived.astype(jnp.float32)
        return sums[0]

    def half_order(self, values, axis):
        if self.halves == 1:
            return values
        width = values.shape[axis] // self.halves
        return jnp.concatenate(
            [
                lax.dynamic_slice_in_dim(values, (self.half ^ at) * width, width, axis)
                for at in range(self.halves)
            ],
            axis=axis,
        )

    def places(self):
        return jnp.stack(
            [mirrored(at ^ self.quarter, self.ranks) for at in range(self.ranks)]
        ).astype(jnp.int32)

    def row_order(self, pieces):
        stacked = jnp.concatenate(pieces, axis=0)
        rows = pieces[0].shape[0]
        return jnp.concatenate(
            [
                lax.dynamic_slice_in_dim(
                    stacked, mirrored(at ^ self.quarter, self.ranks) * rows, rows, 0
                )
                for at in range(self.ranks)
            ],
            axis=0,
        )

    def piece_order(self, values):
        rows = values.shape[0] // self.ranks
        return [
            lax.dynamic_slice_in_dim(
                values, (self.quarter ^ mirrored(at, self.ranks)) * rows, rows, 0
            )
            for at in range(self.ranks)
        ]

    def rank_groups(self):
        return [
            [half * self.ranks + rank for rank in range(self.ranks)] for half in range(self.halves)
        ]

    def spread_ranks(self, shard, hidden_axis):
        return lax.all_to_all(
            shard, "dp", hidden_axis, 1 - hidden_axis, axis_index_groups=self.rank_groups(), tiled=True
        )

    def spread_cols(self, part, hidden_axis):
        return lax.all_gather(part, "tensor", axis=hidden_axis, tiled=True)

    def spread_halves(self, part, hidden_axis):
        parts = {0: part}
        bit = self.halves // 2
        while bit:
            for at in list(parts):
                parts[at | bit] = self.half_pair(parts[at], bit)
            bit //= 2
        return jnp.concatenate([parts[at] for at in range(self.halves)], axis=1 - hidden_axis)

    def collect(self, grad, hidden_axis, *marks):
        other = 1 - hidden_axis
        width = grad.shape[other] // self.halves
        sums = {
            at: lax.slice_in_dim(grad, at * width, (at + 1) * width, axis=other)
            for at in range(self.halves)
        }
        bit = 1
        while bit < self.halves:
            for at in [item for item in sums if item & bit]:
                arrived = self.half_pair(sums.pop(at).astype(jnp.bfloat16), bit)
                if marks:
                    arrived = after(arrived, *marks)
                sums[at ^ bit] = sums[at ^ bit] + arrived.astype(jnp.float32)
            bit *= 2
        part = lax.psum_scatter(
            sums[0].astype(jnp.bfloat16), "tensor", scatter_dimension=hidden_axis, tiled=True
        )
        return lax.all_to_all(
            part, "dp", other, hidden_axis, axis_index_groups=self.rank_groups(), tiled=True
        ).astype(jnp.float32)

    def rank_part(self, values):
        width = values.shape[0] // self.ranks
        return lax.dynamic_slice_in_dim(values, self.rank * width, width, 0)

    def rank_slots(self, values):
        mine = (jnp.arange(self.ranks) == self.rank).astype(values.dtype)
        blocks = values.reshape(self.cols, 1, -1)
        return (blocks * mine[None, :, None]).reshape(-1)


def swapped_on_device(
    mesh,
    tokens,
    segments,
    cotangent,
    ln1_gain,
    ln1_shift,
    w_query,
    b_query,
    w_key,
    w_value,
    b_value,
    w_out,
    b_out,
    ln2_gain,
    ln2_shift,
    w_up,
    b_up,
    w_down,
    b_down,
):
    links = Links(mesh)
    ranks, cols = links.ranks, links.cols
    score_scale = 1.0 / math.sqrt(HDIM)
    head_cols = w_query.shape[1]
    heads_here = head_cols // HDIM
    sub_cols = head_cols // ranks
    f32 = jnp.float32
    low = jnp.bfloat16

    tokens = links.half_order(links.swap(tokens), 1)
    segments = links.swap(segments)

    w_qkv_shard = jnp.concatenate(
        [item.reshape(-1, ranks, sub_cols) for item in (w_query, w_key, w_value)], axis=2
    ).reshape(w_query.shape[0], -1)
    biases = jnp.concatenate([links.rank_part(item) for item in (b_query, b_value, b_up)])
    biases = links.gather_cols(biases.astype(f32))
    bias_query = biases[:, :sub_cols].reshape(-1)
    bias_value = biases[:, sub_cols : 2 * sub_cols].reshape(-1)
    bias_up = biases[:, 2 * sub_cols :].reshape(-1)
    part_qkv = links.spread_ranks(w_qkv_shard, 1)
    part_out, part_up, part_down = (
        links.spread_ranks(after(shard, part_qkv), axis)
        for shard, axis in ((w_out, 0), (w_up, 1), (w_down, 0))
    )
    part_qkv = links.spread_cols(part_qkv, 1)
    full_qkv = links.spread_halves(part_qkv, 1)
    part_out = links.spread_cols(after(part_out, part_qkv), 0)
    part_up = links.spread_cols(after(part_up, part_qkv), 1)
    part_down = links.spread_cols(after(part_down, part_up), 0)
    full_out = links.spread_halves(part_out, 0)

    gain_one, shift_one, gain_two, shift_two, out_bias, down_bias = (
        links.half_order(item.astype(f32), 0)
        for item in (ln1_gain, ln1_shift, ln2_gain, ln2_shift, b_out, b_down)
    )

    inputs = tokens.astype(f32)
    normed_one, norm_one_back = jax.vjp(layer_norm, inputs, gain_one, shift_one)
    h_one_pieces = links.gather_rows(normed_one.astype(low))
    blocks = (heads_here, 1, HDIM)
    no_bias = jnp.zeros(blocks, f32)
    qkv_bias = jnp.concatenate(
        [bias_query.reshape(blocks), no_bias, bias_value.reshape(blocks)], axis=1
    ).reshape(-1)
    qkv_scale = jnp.concatenate(
        [jnp.full(blocks, score_scale, f32), jnp.ones((heads_here, 2, HDIM), f32)], axis=1
    ).reshape(-1)
    qkv = jnp.concatenate(
        [((row_dot(piece, full_qkv) + qkv_bias) * qkv_scale).astype(low) for piece in h_one_pieces],
        axis=0,
    )
    places = links.places()
    grad_y_low = links.half_order(links.swap(after(cotangent, part_qkv)), 1)
    grad_y = grad_y_low.astype(f32)
    grad_y_pieces = links.gather_rows(grad_y_low)
    attended, log_total = attention(places, qkv, segments)
    attended = after(attended, *grad_y_pieces)
    full_up = links.spread_halves(after(part_up, log_total), 1)
    rows = tokens.shape[0]
    attended_pieces = [attended[at * rows : (at + 1) * rows] for at in range(ranks)]
    mixed_pieces = [row_dot(piece, full_out) for piece in attended_pieces]
    resid = (
        inputs
        + links.scatter_rows(mixed_pieces)
        + out_bias
    )
    normed_two, norm_two_back = jax.vjp(layer_norm, resid, gain_two, shift_two)
    h_two = jnp.concatenate(links.gather_rows(normed_two.astype(low)), axis=0)
    full_down = links.spread_halves(after(part_down, resid), 0)
    pre_act = row_dot(h_two, full_up) + bias_up
    activated, gelu_back = jax.vjp(gelu_exact, pre_act)
    act_low = activated.astype(low)
    full_down = after(full_down, act_low)
    grad_y_full = jnp.concatenate(grad_y_pieces, axis=0)
    grad_w_down = left_dot(act_low, grad_y_full)
    grad_act = back_dot(grad_y_full, full_down)
    grad_pre = gelu_back(grad_act)[0].astype(low)
    grad_bias_up = jnp.sum(grad_pre.astype(f32), axis=0)
    grad_w_up = left_dot(h_two, grad_pre)
    up_back_pieces = [
        back_dot(grad_pre[at * rows : (at + 1) * rows], full_up) for at in range(ranks)
    ]
    grad_h_two = links.scatter_rows(up_back_pieces)
    grad_resid_norm, grad_gain_two, grad_shift_two = norm_two_back(grad_h_two)
    grad_resid = grad_y + grad_resid_norm
    grad_mix = grad_resid.astype(low)
    grad_bias_out = jnp.sum(grad_mix.astype(f32), axis=0)
    grad_bias_down = jnp.sum(grad_y, axis=0)

    def summed(*vectors):
        packed = links.total(jnp.concatenate(vectors).reshape(-1, 128)).reshape(-1)
        ends = [sum(item.size for item in vectors[: at + 1]) for at in range(len(vectors))]
        return [packed[end - item.size : end] for item, end in zip(vectors, ends)]

    early = summed(
        links.rank_slots(grad_bias_up),
        links.half_order(grad_gain_two, 0),
        links.half_order(grad_shift_two, 0),
        links.half_order(grad_bias_out, 0),
        links.half_order(grad_bias_down, 0),
    )
    grad_mix_pieces = links.gather_rows(grad_mix)
    grad_mix_full = jnp.concatenate(grad_mix_pieces, axis=0)
    down_pieces = [
        row_dot(act_low[at * rows : (at + 1) * rows], full_down) for at in range(ranks)
    ]
    down_pieces = after(down_pieces, grad_mix_pieces[-1])
    output = (resid + links.scatter_rows(down_pieces) + down_bias).astype(low)
    output = links.swap(links.half_order(output, 1))
    grad_w_out = left_dot(attended, grad_mix_full)
    grad_att = jnp.concatenate(
        [back_dot(piece, full_out).astype(low) for piece in grad_mix_pieces], axis=0
    )
    grad_att = after(grad_att, early)
    grad_qkv, bias_sums = attention_back(places, qkv, grad_att, log_total, segments, score_scale)
    qkv_back_pieces = [
        back_dot(grad_qkv[at * rows : (at + 1) * rows], full_qkv) for at in range(ranks)
    ]
    sent_down = links.collect(grad_w_down, 0, grad_qkv)
    grad_bias_query = bias_sums[:, 0, :HDIM].reshape(-1)
    grad_bias_value = bias_sums[:, 0, HDIM:].reshape(-1)
    grad_w_qkv = left_dot(jnp.concatenate(h_one_pieces, axis=0), grad_qkv)
    sent_up = links.collect(grad_w_up, 1, qkv_back_pieces, grad_w_qkv)
    sent_qkv = links.collect(grad_w_qkv, 1)
    sent_qkv = sent_qkv.reshape(w_query.shape[0], ranks, 3, sub_cols)
    sent_query, sent_key, sent_value = (
        sent_qkv[:, :, at].reshape(w_query.shape) for at in range(3)
    )
    grad_h_one = links.scatter_rows(qkv_back_pieces)
    sent_out = links.collect(grad_w_out, 0, grad_h_one)
    grad_in_norm, grad_gain_one, grad_shift_one = norm_one_back(grad_h_one)
    input_grad = (grad_resid + grad_in_norm).astype(low)
    input_grad = links.swap(links.half_order(input_grad, 1))

    def my_block(values):
        width = values.shape[0] // cols
        return lax.dynamic_slice_in_dim(values, links.col * width, width, 0)

    late = summed(
        links.rank_slots(grad_bias_query),
        links.rank_slots(grad_bias_value),
        links.half_order(grad_gain_one, 0),
        links.half_order(grad_shift_one, 0),
    )
    return (
        output,
        input_grad,
        late[2],
        late[3],
        sent_query,
        my_block(late[0]),
        sent_key,
        sent_value,
        my_block(late[1]),
        sent_out,
        early[3],
        early[1],
        early[2],
        sent_up,
        my_block(early[0]),
        sent_down,
        early[4],
    )


def can_swap(mesh, head_cols):
    ranks = mesh.shape["tensor"]
    dp_size = mesh.shape["dp"]
    if dp_size % ranks or not power_of_two(ranks) or not power_of_two(dp_size // ranks):
        return False
    return head_cols % (ranks * HDIM) == 0


def either_on_device(mesh):
    def run(*arrays):
        w_query = arrays[5]
        if can_swap(mesh, w_query.shape[1]):
            return swapped_on_device(mesh, *arrays)
        return on_device(*arrays)

    return run


def solution(mesh):
    return jax.shard_map(
        either_on_device(mesh),
        mesh=mesh,
        in_specs=(
            P(("dp", "tensor"), None),
            P("dp"),
            P(("dp", "tensor"), None),
            P(),
            P(),
            P("dp", "tensor"),
            P("tensor"),
            P("dp", "tensor"),
            P("dp", "tensor"),
            P("tensor"),
            P("tensor", "dp"),
            P(),
            P(),
            P(),
            P("dp", "tensor"),
            P("tensor"),
            P("tensor", "dp"),
            P(),
        ),
        out_specs=(
            P(("dp", "tensor"), None),
            P(("dp", "tensor"), None),
            P(),
            P(),
            P("dp", "tensor"),
            P("tensor"),
            P("dp", "tensor"),
            P("dp", "tensor"),
            P("tensor"),
            P("tensor", "dp"),
            P(),
            P(),
            P(),
            P("dp", "tensor"),
            P("tensor"),
            P("tensor", "dp"),
            P(),
        ),
        check_vma=False,
    )
```
